128 devices in a mesh: tm: 4 (over z_hi, core), ent: 8 (over y, z_lo), batch: 4 (over x).
Axes of the slice: x: 4, y: 4, z: 4 (z_hi: 2, z_lo: 2; z = z_hi * 2 + z_lo), core: 2. Of those that a mesh axis runs over, the one named last changes fastest.
Arguments:
- init_state: float32 [4, 4096, 256], P('batch', 'ent'), may hold values from -6 to 6
- tiles: float32 [4, 4, 16, 512, 512], P('batch', 'tm', 'ent'), may hold values from -0.25 to 0.25
- dst_block: int32 [4, 4, 16], P('batch', 'tm', 'ent'), may hold values from 0 to 7
- rel_id: int32 [4, 4, 16], P('batch', 'tm', 'ent'), may hold values from 0 to 255
- cotangent: float32 [4, 4, 4096, 256], P('batch', 'tm', 'ent'), may hold values from -0.0625 to 0.0625
- rel_emb: float32 [256, 256], replicated, may hold values from -6 to 6
- w_neigh: float32 [256, 256], replicated, may hold values from -0.1875 to 0.1875
- w_self: float32 [256, 256], replicated, may hold values from -0.375 to 0.375
- w_gate: float32 [256, 256], replicated, may hold values from -0.375 to 0.375
- b_gate: float32 [256], replicated, may hold values from -2 to 2
Outputs:
- states: float32 [4, 4, 4096, 256], P('batch', 'tm', 'ent')
- grad_rel: float32 [256, 256], replicated
- grad_neigh: float32 [256, 256], replicated
- grad_self: float32 [256, 256], replicated
- grad_gate: float32 [256, 256], replicated
- grad_bias: float32 [256], replicated
The draws below stay inside these ranges and needn't reach their ends.
All inputs are finite; a program needn't handle non-finite values.
Results may differ from the reference program's by a relative error of at most 0.00012.
Values sent between devices are 32-bit elements; how exact they have to be, the bound alone decides.
No kernel may reach another device: no remote copies, remote signals or barrier semaphores. Data moves between devices by JAX's collectives and lax.ppermute only.
A program may use at most 64 MiB of HBM per device.

```python
import jax
import jax.numpy as jnp
from jax import lax

D = 256
REL = 256
TILE = 512
TILES_DEV = 2
SNAPS = 4
ENTITIES = 4096
BLOCKS_ALL = 16
WINDOWS = 4
N_ENT = 8
N_BATCH = 4


def set_ends(values, own_key, smallest, high):
    place = [jax.random.randint(jax.random.fold_in(own_key, axis), (), 0, length) for axis, length in enumerate(values.shape)]
    longest = values.shape.index(max(values.shape))
    neighbour = place[:longest] + [(place[longest] + 1) % values.shape[longest]] + place[longest + 1:]
    return values.at[tuple(place)].set(smallest).at[tuple(neighbour)].set(high)


def level_of(rng, shape, cuts, least, high):
    def one(position, blocks):
        draws = jax.random.uniform(jax.random.fold_in(jax.random.fold_in(rng, 6), position), (blocks,), jnp.float32, least / len(cuts), high / len(cuts))
        return jnp.repeat(jnp.exp(draws), shape[position] // blocks).reshape((-1,) + (1,) * (len(shape) - position - 1))

    loudness = one(*cuts[0])
    for cut in cuts[1:]:
        loudness = loudness * one(*cut)
    return loudness


def bell_draw(stream_key, shape, deviation, most, split=(), kind=jnp.bfloat16):
    array = jax.random.normal(stream_key, shape, jnp.float32) * deviation
    if len(split) > 0:
        array = level_of(stream_key, shape, split, -0.22, 0.18) * array
    return jnp.clip(array, min=-most, max=most).astype(kind)


def setup_inputs(seed: int = 0) -> dict:
    arg_keys = jax.random.split(jax.random.key(seed), 11)
    return {
        "init_state": bell_draw(arg_keys[0], (WINDOWS, ENTITIES, D), 1.0, 6.0, ((0, 4), (1, 8)), jnp.float32),
        "tiles": bell_draw(arg_keys[1], (WINDOWS, SNAPS, BLOCKS_ALL, TILE, TILE), TILE ** -0.5, 0.25, ((0, 4), (1, 4), (2, 8)), jnp.float32),
        "dst_block": set_ends(jax.random.randint(arg_keys[2], (WINDOWS, SNAPS, BLOCKS_ALL), 0, N_ENT), jax.random.fold_in(arg_keys[2], 1), 0, N_ENT - 1).astype(jnp.int32),
        "rel_id": set_ends(jax.random.randint(arg_keys[3], (WINDOWS, SNAPS, BLOCKS_ALL), 0, REL), jax.random.fold_in(arg_keys[3], 1), 0, REL - 1).astype(jnp.int32),
        "cotangent": bell_draw(arg_keys[4], (WINDOWS, SNAPS, ENTITIES, D), (1.0 / (SNAPS * ENTITIES * N_BATCH) ** 0.5), 0.0625, ((0, 4), (1, 4), (2, 8)), jnp.float32),
        "rel_emb": bell_draw(arg_keys[5], (REL, D), 1.0, 6.0, (), jnp.float32),
        "w_neigh": bell_draw(arg_keys[6], (D, D), (4 * D) ** -0.5, 0.1875, (), jnp.float32),
        "w_self": bell_draw(arg_keys[7], (D, D), D ** -0.5, 0.375, (), jnp.float32),
        "w_gate": bell_draw(arg_keys[8], (D, D), D ** -0.5, 0.375, (), jnp.float32),
        "b_gate": jnp.clip(jax.random.uniform(arg_keys[9], (D,), jnp.float32, -2.0, 2.0), -2.0, 2.0),
    }


highest = lax.Precision.HIGHEST

def snapshot(current, tiles_t, dst_t, rel_t, params):
    rel_emb, w_neigh, w_self, w_gate, b_gate = params
    held_rows = current.reshape(N_ENT, TILE, D)
    owner_block = jnp.arange(N_ENT * TILES_DEV, dtype=jnp.int32) // TILES_DEV
    source = held_rows[owner_block]
    rows_sum = lax.optimization_barrier(jnp.sum(tiles_t, axis=2))
    result = jnp.einsum('tij,tjd->tid', tiles_t, source, precision=highest)
    result = result + rows_sum[:, :, None] * rel_emb[rel_t][:, None, :]
    dest_pick = (dst_t[:, None] == jnp.arange(N_ENT, dtype=jnp.int32)[None, :]).astype(jnp.float32)
    incoming = jnp.einsum('tg,tid->gid', dest_pick, result, precision=highest).reshape(ENTITIES, D)
    update_gate = jax.nn.sigmoid(jnp.dot(current, w_gate, precision=highest) + b_gate)
    candidate = jnp.tanh(jnp.dot(incoming, w_neigh, precision=highest) + jnp.dot(current, w_self, precision=highest))
    return update_gate * candidate + (1.0 - update_gate) * current

def reference(init_state, tiles, dst_block, rel_id, cotangent, rel_emb, w_neigh, w_self, w_gate, b_gate):
    params = (rel_emb, w_neigh, w_self, w_gate, b_gate)
    all_states = []
    totals = None
    for window in range(WINDOWS):

        def run_window(weights):
            current = init_state[window]
            collected = []
            for snap_index in range(SNAPS):
                current = snapshot(current, tiles[window, snap_index], dst_block[window, snap_index], rel_id[window, snap_index], weights)
                collected.append(current)
            return jnp.stack(collected)
        outputs, pullback = jax.vjp(run_window, params)
        grads_now = pullback(cotangent[window])[0]
        all_states.append(outputs)
        if totals is None:
            totals = grads_now
        else:
            totals = tuple((a + b for a, b in zip(totals, grads_now)))
    return (jnp.stack(all_states), totals[0], totals[1], totals[2], totals[3], totals[4])
```

```python
import jax
import jax.numpy as jnp
from jax import lax
from jax.sharding import Mesh
from jax.sharding import PartitionSpec as P


AXES = ("zh", "c", "y", "zl", "b")
TM = ("zh", "c")
ENT = ("y", "zl")
ROWS = ("zh", "zl", "c")
Z = ("zh", "zl")
highest = lax.Precision.HIGHEST


def product(left, right):
    return jnp.dot(left, right, precision=highest)


def along(value, axis, steps):
    count = lax.axis_size(axis)
    return lax.ppermute(value, axis, [(i, (i + steps) % count) for i in range(count)])


def pick(stack, index):
    return lax.dynamic_index_in_dim(stack, index, 0, keepdims=False)


def on_device(
    init_state, tiles, dst_block, rel_id, cotangent, rel_emb, w_neigh, w_self, w_gate, b_gate
):
    z, c, y = lax.axis_index(Z), lax.axis_index("c"), lax.axis_index("y")
    n_y, n_z, n_c = lax.axis_size("y"), lax.axis_size(Z), 2
    n_r = n_z * n_c
    snaps = lax.axis_size("zh") * n_c
    tile, width = init_state.shape[1:]
    rows = tile // n_r
    r = z * n_c + c

    ids = lax.all_gather(jnp.stack([dst_block[0, 0], rel_id[0, 0]]), TM + ENT, axis=0)
    ids = ids.reshape(snaps, 2 * n_y, 2, 2).transpose(2, 0, 1, 3).reshape(2, snaps, 4 * n_y)
    dst, rel = ids[0], ids[1]

    blocks = tiles[0, 0].reshape(2, n_r, rows, tile).transpose(1, 0, 2, 3)
    got = lax.all_to_all(blocks, ROWS, 0, 0, tiled=True)
    got = got.reshape(2, 2, 2, 2, rows, tile).transpose(0, 2, 1, 3, 4, 5).reshape(snaps, 4, rows, tile)
    cot = lax.all_to_all(cotangent[0, 0].reshape(n_r, rows, width), ROWS, 0, 0, tiled=True)
    cot = cot.reshape(2, 2, 2, rows, width).transpose(0, 2, 1, 3, 4).reshape(snaps, 2 * rows, width)

    mate = along(init_state[0], "zl", 1)
    first = lax.axis_index("zl") == 0
    full = jnp.stack([jnp.where(first, init_state[0], mate), jnp.where(first, mate, init_state[0])])
    own = pick(full.reshape(2, n_r, rows, width).transpose(1, 0, 2, 3), r).reshape(2 * rows, width)

    sums = jnp.sum(got, axis=3)
    sums_y = [sums] + [along(sums, "y", s) for s in (1, 2, 3)]
    all_sums = jnp.stack([pick(jnp.stack(sums_y), (y - i) % n_y) for i in range(n_y)], axis=1)
    all_sums = all_sums.reshape(snaps, 4 * n_y, rows)
    here = (dst[:, :, None] == (2 * y + jnp.arange(2, dtype=jnp.int32))[None, None, :]).astype(jnp.float32)
    coef = (here[:, :, :, None] * all_sums[:, :, None, :]).reshape(snaps, 4 * n_y, 2 * rows)
    rel_pick = (rel[:, :, None] == jnp.arange(rel_emb.shape[0], dtype=jnp.int32)).astype(jnp.float32)
    rel_rows = jnp.einsum("tkr,rd->tkd", rel_pick, rel_emb, precision=highest)
    rel_term = jnp.einsum("tki,tkd->tid", coef, rel_rows, precision=highest)

    my_dst = lax.dynamic_slice_in_dim(dst, 4 * y, 4, 1)
    where_to = (2 * ((y + jnp.arange(n_y)[:, None]) % n_y) + jnp.arange(2)[None, :]).astype(jnp.int32)
    route = (my_dst[:, :, None, None] == where_to[None, None]).astype(jnp.float32)

    state, stored, states_out = own, [], []
    for t in range(snaps):
        part = jnp.einsum(
            "bkij,bjd->bkid", got[t].reshape(2, 2, rows, tile), full, precision=highest
        ).reshape(4, rows, width)
        to_y = [
            sum(route[t, k, s].reshape(2, 1, 1) * part[k][None] for k in range(4)) for s in range(n_y)
        ]
        agg = to_y[0]
        for s in range(1, n_y):
            agg = agg + along(to_y[s], "y", s)
        agg = agg.reshape(2 * rows, width) + rel_term[t]
        update = jax.nn.sigmoid(product(state, w_gate) + b_gate)
        candidate = jnp.tanh(product(agg, w_neigh) + product(state, w_self))
        new = update * candidate + (1.0 - update) * state
        stored.append((state, agg, update, candidate))
        states_out.append(new)
        state = new
        if t + 1 < snaps:
            column = jnp.stack([new] + [along(new, Z, s) for s in range(1, n_z)])
            other = along(column, "c", 1)
            pair = jnp.stack([column, other])
            absolute = jnp.stack(
                [pick(pick(pair, (c != cc).astype(jnp.int32)), (z - zz) % n_z) for zz in range(n_z) for cc in range(2)]
            )
            full = absolute.reshape(n_r, 2, rows, width).transpose(1, 0, 2, 3).reshape(2, tile, width)

    out = jnp.stack(states_out).reshape(2, 2, 2, rows, width).transpose(0, 2, 1, 3, 4)
    state_out = lax.all_to_all(out.reshape(n_r, rows, width), ROWS, 0, 0, tiled=True).reshape(1, 1, tile, width)

    carry = None
    kept = []
    for t in reversed(range(snaps)):
        state, agg, update, candidate = stored[t]
        d_new = cot[t] if carry is None else cot[t] + carry
        d_pre = d_new * update * (1.0 - candidate * candidate)
        d_gate = d_new * (candidate - state) * update * (1.0 - update)
        d_agg = product(d_pre, w_neigh.T)
        kept.append((state, agg, d_pre, d_gate, d_agg))
        if t == 0:
            break
        d_prev = d_new * (1.0 - update) + product(d_pre, w_self.T) + product(d_gate, w_gate.T)
        pieces = d_agg.reshape(2, rows, width)
        from_y = [pieces] + [along(pieces, "y", -s) for s in range(1, n_y)]
        d_res = [
            sum(route[t, k, s, bl] * from_y[s][bl] for s in range(n_y) for bl in range(2)) for k in range(4)
        ]
        d_full = jnp.einsum(
            "bkij,bkid->bjd",
            got[t].reshape(2, 2, rows, tile),
            jnp.stack(d_res).reshape(2, 2, rows, width),
            precision=highest,
        )
        by_c = d_full.reshape(2, n_z, n_c, rows, width).transpose(2, 1, 0, 3, 4)
        mine = pick(by_c, c) + along(pick(by_c, 1 - c), "c", 1)
        d_own = pick(mine, z)
        for s in range(1, n_z):
            d_own = d_own + along(pick(mine, (z + s) % n_z), Z, s)
        carry = d_prev + d_own.reshape(2 * rows, width)

    kept = kept[::-1]
    state_all, agg_all, pre_all, gate_all = (jnp.concatenate([k[i] for k in kept]) for i in range(4))
    d_neigh = product(agg_all.T, pre_all)
    d_self = product(state_all.T, pre_all)
    d_gate_w = product(state_all.T, gate_all)
    d_bias = jnp.sum(gate_all, axis=0)
    d_agg_all = jnp.stack([k[4] for k in kept])
    picked = jnp.einsum("tki,tid->tkd", coef, d_agg_all, precision=highest)
    d_rel = jnp.einsum("tkr,tkd->rd", rel_pick, picked, precision=highest)

    n_all = lax.axis_size(AXES)
    packed = jnp.concatenate([d_rel, d_neigh, d_self, d_gate_w]).reshape(n_all, 8, width)
    bias = jnp.pad(d_bias.reshape(n_all, 1, 2), ((0, 0), (0, 7), (0, 126)))
    packed = jnp.concatenate([packed, bias], axis=2)
    summed = jnp.sum(lax.all_to_all(packed, AXES, 0, 0, tiled=True), axis=0)
    spread = lax.all_to_all(jnp.broadcast_to(summed[None], packed.shape), AXES, 0, 0, tiled=True)
    totals = spread[:, :, :width].reshape(4, -1, width)
    return (state_out, totals[0], totals[1], totals[2], totals[3], spread[:, 0, width : width + 2].reshape(-1))


def solution(mesh):
    torus = Mesh(mesh.devices.reshape(2, 2, 4, 2, mesh.shape["batch"]), AXES)
    return jax.shard_map(
        on_device,
        mesh=torus,
        in_specs=(
            P("b", ENT, None),
            P("b", TM, ENT, None, None),
            P("b", TM, ENT),
            P("b", TM, ENT),
            P("b", TM, ENT, None),
            P(),
            P(),
            P(),
            P(),
            P(),
        ),
        out_specs=(P("b", TM, ENT, None), P(), P(), P(), P(), P()),
        check_vma=False,
    )
```

```python
import functools

import jax
import jax.numpy as jnp
from jax import lax
from jax.experimental import pallas as pl
from jax.experimental.pallas import tpu as pltpu
from jax.sharding import Mesh
from jax.sharding import PartitionSpec as P

INTERPRET = False
VMEM_LIMIT = 16 * 1024 * 1024

AXES = ("zh", "c", "y", "zl", "b")
CHIPS = ("zh", "zl", "y", "b")
TM = ("zh", "c")
ENT = ("y", "zl")
Z = ("zh", "zl")
highest = lax.Precision.HIGHEST
F32 = jnp.float32


def product(left, right, dims=((1,), (0,))):
    return lax.dot_general(left, right, (dims, ((), ())), precision=highest, preferred_element_type=F32)


def along(value, axis, steps):
    count = lax.axis_size(axis)
    return lax.ppermute(value, axis, [(i, (i + steps) % count) for i in range(count)])


def swap(value):
    return along(value, "c", 1)


def order(value, after):
    return lax.optimization_barrier((value, after))[0]


def local(kernel, name, place, arrays, outs, scratch=(), flops=1_000_000):
    vmem = pl.BlockSpec(memory_space=pltpu.VMEM)
    size = sum(a.size for a in arrays) + sum(functools.reduce(lambda p, q: p * q, o) for o in outs)
    return pl.pallas_call(
        kernel,
        out_shape=[jax.ShapeDtypeStruct(o, F32) for o in outs],
        in_specs=[pl.BlockSpec(memory_space=pltpu.SMEM)] + [vmem] * len(arrays),
        out_specs=[vmem] * len(outs),
        scratch_shapes=[pltpu.VMEM(s, F32) for s in scratch],
        cost_estimate=pl.CostEstimate(flops=flops, bytes_accessed=4 * size, transcendentals=0),
        compiler_params=pltpu.CompilerParams(vmem_limit_bytes=VMEM_LIMIT),
        name=name,
        interpret=INTERPRET,
    )(place, *arrays)


def slot_at(place, t, k):
    return place[4 + 4 * t + k]


def rel_at(place, t, k):
    return place[20 + 4 * t + k]


def ahead(z, s):
    return lax.rem(z + s, 4)


def behind(z, s):
    return lax.rem(z + 4 - s, 4)


def row(i, step):
    return pl.multiple_of(i * step, step)


def cut_tiles(place, own, got, *outs):
    z, c = place[0], place[1]
    rows = got.shape[2]
    for s in range(4):
        to = ahead(z, s)
        for j in range(2):
            mine = own[j, pl.ds(row(to * 2 + c, rows), rows), :]
            other = got[j, to]
            outs[s][j] = jnp.where(c == 0, mine, other)
            outs[4 + s][j] = jnp.where(c == 0, other, mine)


def join_tiles(place, p0, p1, p2, p3, early, late, stack):
    z = place[0]
    rows = p0.shape[1]
    for s, piece in enumerate((p0, p1, p2, p3)):
        stack[behind(z, s)] = piece[...].reshape(2 * rows, -1)
    early[...] = stack[0:2]
    late[...] = stack[2:4]


def spread(place, t, tiles, rel_emb, full, slots, outs):
    rows = outs[0].shape[1]
    slots[...] = jnp.zeros_like(slots)
    for b in range(2):
        block = tiles[b]
        part = product(block, full[b])
        sums = jnp.sum(block, axis=1, keepdims=True)
        for j in range(2):
            k = 2 * b + j
            line = rel_emb[pl.ds(rel_at(place, t, k), 1), :]
            slots[slot_at(place, t, k)] += (
                part[j * rows : (j + 1) * rows] + sums[j * rows : (j + 1) * rows] * line
            )
    for s in range(4):
        outs[s][...] = slots[2 * s : 2 * s + 2]


def spread_first(place, tiles, rel_emb, init, near, far, o0, o1, o2, o3, own, full, slots):
    z, c, zl = place[0], place[1], place[2]
    half = near.shape[0]
    rows = o0.shape[1]
    full[zl] = init[...]
    full[1 - zl, pl.ds(row(c, half), half), :] = near[...]
    full[1 - zl, pl.ds(row(1 - c, half), half), :] = far[...]
    at = row(z * 2 + c, rows)
    for b in range(2):
        own[b * rows : (b + 1) * rows, :] = full[b, pl.ds(at, rows), :]
    spread(place, 0, tiles, rel_emb, full, slots, (o0, o1, o2, o3))


def spread_next(t, place, tiles, rel_emb, *refs):
    pieces, outs, (full, slots) = refs[:8], refs[8:12], refs[12:]
    z, c = place[0], place[1]
    rows = outs[0].shape[1]
    for s in range(4):
        from_z = behind(z, s)
        for b in range(2):
            part = pl.ds(b * rows, rows)
            full[b, pl.ds(row(from_z * 2 + c, rows), rows), :] = pieces[s][part, :]
            full[b, pl.ds(row(from_z * 2 + 1 - c, rows), rows), :] = pieces[4 + s][part, :]
    spread(place, t, tiles, rel_emb, full, slots, outs)


def gates(place, state, w_self, w_gate, b_gate, update, self_part):
    held = state[...]
    update[...] = jax.nn.sigmoid(product(held, w_gate[...]) + b_gate[...])
    self_part[...] = product(held, w_self[...])


def advance(place, a0, a1, a2, a3, state, update, self_part, w_neigh, new, agg, candidate):
    total = ((a0[...] + a1[...]) + (a2[...] + a3[...])).reshape(agg.shape)
    agg[...] = total
    cand = jnp.tanh(product(total, w_neigh[...]) + self_part[...])
    candidate[...] = cand
    gate = update[...]
    new[...] = gate * cand + (1.0 - gate) * state[...]


def retreat_math(d_new, state, update, candidate, w_neigh, d_pre, d_gate, d_agg, d_keep):
    gate, cand = update[...], candidate[...]
    rest = 1.0 - gate
    pre = d_new * gate * (1.0 - cand * cand)
    d_pre[...] = pre
    d_gate[...] = d_new * (cand - state[...]) * gate * rest
    d_agg[...] = product(pre, w_neigh[...], ((1,), (1,))).reshape(d_agg.shape)
    if d_keep is not None:
        d_keep[...] = d_new * rest


def retreat_last(place, cot, state, update, candidate, w_neigh, d_pre, d_gate, d_agg, d_keep):
    d_new = cot[...].reshape(state.shape)
    retreat_math(d_new, state, update, candidate, w_neigh, d_pre, d_gate, d_agg, d_keep)


def retreat(place, d0, d1, d2, d3, d_prev, cot, state, update, candidate, w_neigh, d_pre, d_gate, d_agg, d_keep):
    came = ((d0[...] + d1[...]) + (d2[...] + d3[...]) + cot[...]).reshape(state.shape)
    retreat_math(came + d_prev[...], state, update, candidate, w_neigh, d_pre, d_gate, d_agg, d_keep)


def before(place, d_keep, d_pre, d_gate, w_self, w_gate, d_prev):
    d_prev[...] = (
        d_keep[...]
        + product(d_pre[...], w_self[...], ((1,), (1,)))
        + product(d_gate[...], w_gate[...], ((1,), (1,)))
    )


def gather_back(t, place, tiles, g0, g1, g2, g3, other, mine, rel_rows, held, res, full):
    z, c = place[0], place[1]
    rows = g0.shape[1]
    for s, piece in enumerate((g0, g1, g2, g3)):
        held[2 * s : 2 * s + 2] = piece[...]
    rel_rows[...] = jnp.zeros_like(rel_rows)
    for b in range(2):
        block = tiles[b]
        sums = jnp.sum(block, axis=1, keepdims=True)
        for j in range(2):
            k = 2 * b + j
            value = held[slot_at(place, t, k)]
            res[b, j * rows : (j + 1) * rows, :] = value
            rel_rows[k : k + 1, :] = jnp.sum(sums[j * rows : (j + 1) * rows] * value, axis=0, keepdims=True)
        full[b] = product(block, res[b], ((0,), (0,)))
    for s in range(4):
        to = ahead(z, s)
        for b in range(2):
            mine[s, b] = full[b, pl.ds(row(to * 2 + c, rows), rows), :]
            other[s, b] = full[b, pl.ds(row(to * 2 + 1 - c, rows), rows), :]


def add_pairs(place, mine, got, n0, n1, n2, n3):
    for s, out in enumerate((n0, n1, n2, n3)):
        out[...] = mine[s] + got[s]


def cut_rows(place, own, got, *outs):
    z, c = place[0], place[1]
    rows = got.shape[1]
    for s in range(4):
        to = ahead(z, s)
        outs[s][c] = own[pl.ds(row(to * 2 + c, rows), rows), :]
        outs[s][1 - c] = got[to]


def join_rows(place, p0, p1, p2, p3, *refs):
    outs, stack = refs[:4], refs[4]
    z = place[0]
    for s, piece in enumerate((p0, p1, p2, p3)):
        stack[behind(z, s)] = piece[...]
    for t in range(4):
        for b in range(2):
            outs[t][b] = stack[(t // 2) * 2 + b, t % 2]


def cut_states(place, n0, n1, n2, n3, *refs):
    outs, stack = refs[:4], refs[4]
    z = place[0]
    rows = outs[0].shape[1]
    for t, state in enumerate((n0, n1, n2, n3)):
        for b in range(2):
            stack[(t // 2) * 2 + b, t % 2] = state[b * rows : (b + 1) * rows, :]
    for s in range(4):
        outs[s][...] = stack[ahead(z, s)]


def sort_states(place, p0, p1, p2, p3, mine, other):
    c = place[1]
    for s, piece in enumerate((p0, p1, p2, p3)):
        mine[s] = piece[c]
        other[s] = piece[1 - c]


def join_states(place, mine, got, out):
    z, c = place[0], place[1]
    rows = mine.shape[1]
    for s in range(4):
        from_z = behind(z, s)
        out[pl.ds(row(from_z * 2 + c, rows), rows), :] = mine[s]
        out[pl.ds(row(from_z * 2 + 1 - c, rows), rows), :] = got[s]


def row_sums(place, tiles, out):
    rows = tiles.shape[1] // 2
    ones = jnp.ones((8, tiles.shape[2]), F32)
    lane = lax.broadcasted_iota(jnp.int32, (1, 128), 1)
    out[...] = jnp.full(out.shape, -1.0, F32)
    for k in range(4):
        sums = product(ones, tiles[k // 2, (k % 2) * rows : (k % 2 + 1) * rows, :], ((1,), (1,)))
        slot = slot_at(place, 0, k).astype(F32)
        rel = rel_at(place, 0, k).astype(F32)
        out[k : k + 1, :] = jnp.where(lane == rows, slot, jnp.where(lane == rows + 1, rel, 0.0))
        out[k : k + 1, 0:rows] = sums[0:1]


def dense_grads(states, aggs, pres, gates_in):
    total = []
    for left, right in ((aggs, pres), (states, pres), (states, gates_in)):
        total.append(sum(product(a[...], b[...], ((0,), (0,))) for a, b in zip(left, right)))
    return total, sum(jnp.sum(g[...], axis=0, keepdims=True) for g in gates_in)


def later_grads(count, place, *refs):
    states, aggs, pres, gates_in, rel_lines = (refs[i * count : (i + 1) * count] for i in range(5))
    d_rel, d_neigh, d_self, d_gate, d_bias = refs[5 * count :]
    total, bias = dense_grads(states, aggs, pres, gates_in)
    d_rel[...] = jnp.zeros_like(d_rel)
    for i, lines in enumerate(rel_lines):
        for k in range(4):
            d_rel[pl.ds(rel_at(place, i + 1, k), 1), :] += lines[k : k + 1, :]
    for out, value in zip((d_neigh, d_self, d_gate), total):
        out[...] = value
    d_bias[...] = jnp.broadcast_to(bias, d_bias.shape)


def weight_grads(place, state, agg, pre, gate_in, d_agg, l0, l1, l2, l3, *refs):
    later, d_bias, keep, give, stack = refs[:4], refs[4], refs[5], refs[6], refs[7]
    c = place[1]
    rows, width = d_agg.shape[1:]
    total, bias = dense_grads([state], [agg], [pre], [gate_in])
    d_rel = later[0][...]
    relation = lax.broadcasted_iota(jnp.int32, (8, width), 1).astype(F32)
    for s, line in enumerate((l0, l1, l2, l3)):
        slot, rel, sums = line[:, rows : rows + 1], line[:, rows + 1 : rows + 2], line[:, 0:rows]
        found = sum(
            product(jnp.where(slot == float(2 * s + b), sums, 0.0), d_agg[b]) for b in range(2)
        )
        d_rel = d_rel + product((rel == relation).astype(F32), found, ((0,), (0,)))
    total = [d_rel] + [a + b[...] for a, b in zip(total, later[1:])]
    bias = bias + d_bias[0:1, :]
    stack[...] = jnp.zeros_like(stack)
    chunk = 8
    for half in range(2):
        for i in range(2):
            stack[half, i * width // chunk : (i + 1) * width // chunk, :, 0:width] = total[2 * half + i].reshape(
                width // chunk, chunk, width
            )
        stack[half, 0, 0:1, width:] = bias[:, half * (width // 2) : (half + 1) * (width // 2)]
    keep[...] = stack[c]
    give[...] = stack[1 - c]


def on_device(
    init_state, tiles, dst_block, rel_id, cotangent, rel_emb, w_neigh, w_self, w_gate, b_gate
):
    z, c, y, zl = lax.axis_index(Z), lax.axis_index("c"), lax.axis_index("y"), lax.axis_index("zl")
    snaps = 4
    tile, width = init_state.shape[1:]
    rows = tile // 8
    bias_row = b_gate.reshape(1, width)
    pair = (2, rows, width)
    flat = (2 * rows, width)

    own_tiles, own_cot, init = tiles[0, 0], cotangent[0, 0], init_state[0]
    give = lax.dynamic_index_in_dim(own_tiles.reshape(2, 4, 2, rows, tile), 1 - c, 2, keepdims=False)
    got_tiles = swap(give)
    near = along(lax.dynamic_slice_in_dim(init, c * (tile // 2), tile // 2, 0), "zl", 1)

    here = jnp.stack([z, c, zl, y]).astype(jnp.int32)
    piece = (2, rows, tile)
    cut = local(cut_tiles, "cut_tiles", here, (own_tiles, got_tiles), [piece] * 8)
    first_sent = cut[0]
    far = swap(order(near, first_sent))
    ids = order(jnp.stack([dst_block[0, 0], rel_id[0, 0]]), first_sent)
    ids_c = swap(ids)
    ids = jnp.where(c == 0, jnp.stack([ids, ids_c]), jnp.stack([ids_c, ids]))
    ids = jnp.stack([ids] + [along(ids, Z, s) for s in range(1, 4)])
    steps = jnp.arange(4, dtype=jnp.int32)
    came = (jnp.remainder(z - steps[:, None], 4) == steps[None, :]).astype(jnp.int32)
    ids = jnp.sum(came.reshape(4, 4, 1, 1, 1) * ids[None], axis=1)
    ids = ids.reshape(2, 2, 2, 2, 2).transpose(3, 0, 2, 1, 4).reshape(2, snaps, 4)
    dst, rel = ids[0], ids[1]
    slots = jnp.remainder(dst // 2 - y, 4) * 2 + jnp.remainder(dst, 2)
    place = jnp.concatenate([jnp.stack([z, c, zl, y]).astype(jnp.int32), slots.reshape(-1), rel.reshape(-1)])

    held = [None] * snaps
    for core in range(2):
        part = cut[4 * core : 4 * core + 4]
        part = [part[0]] + [along(part[s], Z, s) for s in range(1, 4)]
        held[core], held[2 + core] = local(
            join_tiles, "join_tiles", here, part, [(2, 2 * rows, tile)] * 2, [(4, 2 * rows, tile)]
        )

    work = [(2, tile, width), (8, rows, width)]
    stored, states, sent = [], [], []
    state = None
    for t in range(snaps):
        if t == 0:
            *to_y, state = local(
                spread_first, "spread_0", place, (held[0], rel_emb, init, near, far), [pair] * 4 + [flat], work
            )
        else:
            ring = [state] + [along(state, Z, s) for s in range(1, 4)]
            to_y = local(
                functools.partial(spread_next, t),
                f"spread_{t}",
                place,
                [held[t], rel_emb] + ring + [swap(p) for p in ring],
                [pair] * 4,
                work,
            )
        sent.append(to_y[0])
        if t == 1:
            (line,) = local(row_sums, "row_sums", place, (order(held[0], to_y[0]),), [(8, 128)])
            lines = order([line] + [along(line, "y", s) for s in range(1, 4)], to_y[0])
        if t == 2:
            held[3], lines = lax.optimization_barrier((held[3], lines))
        came_y = [to_y[0]] + [along(to_y[s], "y", s) for s in range(1, 4)]
        update, self_part = local(gates, "gates", here, (state, w_self, w_gate, bias_row), [flat] * 2)
        new, agg, candidate = local(
            advance, "advance", here, came_y + [state, update, self_part, w_neigh], [flat] * 3
        )
        stored.append((state, agg, update, candidate))
        states.append(new)
        state = new

    own_cot = order(own_cot, sent[1])
    give_cot = lax.dynamic_index_in_dim(own_cot.reshape(4, 2, rows, width), 1 - c, 1, keepdims=False)
    cut = local(cut_rows, "cut_rows", here, (own_cot, swap(give_cot)), [pair] * 4)
    cots = local(
        join_rows,
        "join_rows",
        here,
        order([cut[0]] + [along(cut[s], Z, s) for s in range(1, 4)], sent[2]),
        [pair] * 4,
        [(4, 2, rows, width)],
    )

    cut = local(cut_states, "cut_states", here, states, [pair] * 4, [(4, 2, rows, width)])
    cut = [cut[0]] + [along(cut[s], Z, s) for s in range(1, 4)]
    held[3], cut = lax.optimization_barrier((held[3], cut))
    mine_states, other_states = local(sort_states, "sort_states", here, cut, [(4, rows, width)] * 2)
    (state_out,) = local(join_states, "join_states", here, (mine_states, swap(other_states)), [(tile, width)])
    held[2], state_out = lax.optimization_barrier((held[2], state_out))

    d_prev = d_in = out_pieces = None
    pres, gates_in, rel_lines = [None] * snaps, [None] * snaps, []
    for t in reversed(range(snaps)):
        held_state, agg, update, candidate = stored[t]
        tail = (cots[t], held_state, update, candidate, w_neigh)
        outs = [flat, flat, pair, flat]
        if d_in is None:
            d_pre, d_gate, d_agg, d_keep = local(retreat_last, "retreat_last", here, tail, outs)
        else:
            d_pre, d_gate, d_agg, d_keep = local(retreat, "retreat", here, (*d_in, d_prev, *tail), outs)
        pres[t], gates_in[t] = d_pre, d_gate
        if t == 0:
            break
        pieces = [d_agg] + [along(d_agg, "y", -s) for s in range(1, 4)]
        (d_prev,) = local(before, "before", here, (d_keep, d_pre, d_gate, w_self, w_gate), [flat])
        other, mine_rows, rel_rows = local(
            functools.partial(gather_back, t),
            f"gather_back_{t}",
            place,
            [held[t]] + pieces,
            [(4, *pair), (4, *pair), (8, width)],
            [(8, rows, width), (2, 2 * rows, width), (2, tile, width)],
        )
        rel_lines.append(rel_rows)
        if t == 1:
            square = (width, width)
            later = local(
                functools.partial(later_grads, snaps - 1),
                "later_grads",
                place,
                [s[0] for s in stored[1:]]
                + [s[1] for s in stored[1:]]
                + pres[1:]
                + gates_in[1:]
                + rel_lines[::-1],
                [square] * 4 + [(8, width)],
                flops=20_000_000_000,
            )
        parts = local(add_pairs, "add_pairs", here, (mine_rows, swap(other)), [pair] * 4)
        d_in = [parts[0]] + [along(parts[s], Z, s) for s in range(1, 4)]

    size = (64, 8, width + width // 2)
    keep, give = local(
        weight_grads,
        "weight_grads",
        here,
        (stored[0][0], stored[0][1], d_pre, d_gate, d_agg, *lines, *later),
        [size] * 2,
        [(2, *size)],
    )
    packed = keep + swap(give)
    summed = jnp.sum(lax.all_to_all(packed, CHIPS, 0, 0, tiled=True), axis=0)
    mine_sum = lax.all_to_all(jnp.broadcast_to(summed[None], size), CHIPS, 0, 0, tiled=True)
    other_sum = swap(mine_sum)
    halves = (jnp.where(c == 0, mine_sum, other_sum), jnp.where(c == 0, other_sum, mine_sum))
    grads = [h[:, :, :width].reshape(2, width, width)[i] for h in halves for i in range(2)]
    bias = jnp.concatenate([h[0, 0, width:] for h in halves])
    return (state_out.reshape(1, 1, tile, width), *grads, bias)


def solution(mesh):
    torus = Mesh(mesh.devices.reshape(2, 2, 4, 2, mesh.shape["batch"]), AXES)
    return jax.shard_map(
        on_device,
        mesh=torus,
        in_specs=(
            P("b", ENT, None),
            P("b", TM, ENT, None, None),
            P("b", TM, ENT),
            P("b", TM, ENT),
            P("b", TM, ENT, None),
            P(),
            P(),
            P(),
            P(),
            P(),
        ),
        out_specs=(P("b", TM, ENT, None), P(), P(), P(), P(), P()),
        check_vma=False,
    )
```

```python
import functools
import math

import jax
import jax.numpy as jnp
from jax import lax
from jax.experimental import pallas as pl
from jax.experimental.pallas import tpu as pltpu
from jax.sharding import Mesh
from jax.sharding import PartitionSpec as P


INTERPRET = False
VMEM_LIMIT = 16 * 1024 * 1024

AXES = ("zh", "c", "y", "zl", "b")
TM = ("zh", "c")
ENT = ("y", "zl")
Z = ("zh", "zl")
highest = lax.Precision.HIGHEST
F32 = jnp.float32


def product(left, right, dims=((1,), (0,))):
    return lax.dot_general(left, right, (dims, ((), ())), precision=highest, preferred_element_type=F32)


def along(value, axis, steps):
    count = lax.axis_size(axis)
    return lax.ppermute(value, axis, [(i, (i + steps) % count) for i in range(count)])


def swap(value):
    return along(value, "c", 1)


def order(value, after):
    return lax.optimization_barrier((value, after))[0]


def local(kernel, tables, arrays, outs, scratch=(), flops=1_000_000):
    vmem, smem = pl.BlockSpec(memory_space=pltpu.VMEM), pl.BlockSpec(memory_space=pltpu.SMEM)
    size = sum(a.size for a in arrays) + sum(math.prod(o) for o in outs if not isinstance(o, int))
    return pl.pallas_call(
        kernel,
        out_shape=[
            jax.ShapeDtypeStruct((o,), jnp.int32) if isinstance(o, int) else jax.ShapeDtypeStruct(o, F32)
            for o in outs
        ],
        in_specs=[smem] * len(tables) + [vmem] * len(arrays),
        out_specs=[smem if isinstance(o, int) else vmem for o in outs],
        scratch_shapes=[pltpu.VMEM(s, F32) for s in scratch],
        cost_estimate=pl.CostEstimate(flops=flops, bytes_accessed=4 * size, transcendentals=0),
        compiler_params=pltpu.CompilerParams(vmem_limit_bytes=VMEM_LIMIT),
        interpret=INTERPRET,
    )(*tables, *arrays)


def ahead(z, s):
    return lax.rem(z + s, 4)


def behind(z, s):
    return lax.rem(z + 4 - s, 4)


def row(i, step):
    return pl.multiple_of(i * step, step)


def give_tiles(place, dst, rel, own, init, cot, out, half):
    c = place[1]
    rows = own.shape[1] // 8
    lane = lax.broadcasted_iota(jnp.int32, (8, own.shape[2]), 1) // 128
    codes = jnp.zeros(lane.shape, F32)
    for j in range(2):
        codes = jnp.where(lane == 2 * j, dst[j].astype(F32), codes)
        codes = jnp.where(lane == 2 * j + 1, rel[j].astype(F32), codes)
    for to in range(4):
        for j in range(2):
            out[to, j * rows : (j + 1) * rows, :] = own[j, pl.ds(row(to * 2 + 1 - c, rows), rows), :]
        out[to, 2 * rows : 2 * rows + 8, :] = codes
        lines = cot[pl.ds(row(to * 2 + 1 - c, rows), rows), :]
        out[to, 2 * rows + 8 :, 0 : cot.shape[1]] = lines[0 : rows // 2]
        out[to, 2 * rows + 8 :, cot.shape[1] :] = lines[rows // 2 :]
    half[...] = init[pl.ds(row(c, half.shape[0]), half.shape[0]), :]


def cut_tiles(core, place, dst, rel, own, got, *outs):
    z, c = place[0], place[1]
    rows = own.shape[1] // 8
    lane = lax.broadcasted_iota(jnp.int32, (8, own.shape[2]), 1) // 128

    @pl.when(c == core)
    def _():
        codes = jnp.zeros(lane.shape, F32)
        for j in range(2):
            codes = jnp.where(lane == 2 * j, dst[j].astype(F32), codes)
            codes = jnp.where(lane == 2 * j + 1, rel[j].astype(F32), codes)
        for s in range(4):
            to = ahead(z, s)
            for j in range(2):
                outs[s][j * rows : (j + 1) * rows, :] = own[j, pl.ds(row(to * 2 + c, rows), rows), :]
            outs[s][2 * rows :, :] = codes

    @pl.when(c != core)
    def _():
        for s in range(4):
            outs[s][...] = got[ahead(z, s), 0 : 2 * rows + 8, :]


def join_tiles(place, p0, p1, p2, p3, early, late, early_ids, late_ids):
    z, y = place[0], place[3]
    rows = early.shape[1]
    for s, piece in enumerate((p0, p1, p2, p3)):
        from_z = behind(z, s)
        b = lax.rem(from_z, 2)

        def write(tiles, ids):
            tiles[b] = piece[0:rows, :]
            for j in range(2):
                dst, rel = (
                    jnp.max(piece[rows : rows + 8, (2 * j + i) * 128 : (2 * j + i + 1) * 128]).astype(jnp.int32)
                    for i in range(2)
                )
                ids[2 * b + j] = lax.rem(lax.div(dst, 2) + 4 - y, 4) * 2 + lax.rem(dst, 2)
                ids[4 + 2 * b + j] = rel

        pl.when(from_z < 2)(functools.partial(write, early, early_ids))
        pl.when(from_z >= 2)(functools.partial(write, late, late_ids))


def spread(ids, tiles, rel_emb, full, slots):
    rows = tiles.shape[1] // 2
    slots[...] = jnp.zeros_like(slots)

    def step(b, carry):
        block = tiles[b]
        part = product(block, full[b])
        sums = jnp.sum(block, axis=1, keepdims=True)
        for j in range(2):
            line = rel_emb[pl.ds(ids[4 + 2 * b + j], 1), :]
            slots[ids[2 * b + j]] += part[j * rows : (j + 1) * rows] + sums[j * rows : (j + 1) * rows] * line
        return carry

    lax.fori_loop(0, 2, step, 0)


def spread_first(place, ids, tiles, rel_emb, init, near, far, o0, o1, o2, o3, own, full, slots):
    z, c, zl = place[0], place[1], place[2]
    half = near.shape[0]
    rows = tiles.shape[1] // 2
    full[zl] = init[...]
    full[1 - zl, pl.ds(row(c, half), half), :] = near[...]
    full[1 - zl, pl.ds(row(1 - c, half), half), :] = far[...]
    at = row(z * 2 + c, rows)
    for b in range(2):
        own[b * rows : (b + 1) * rows, :] = full[b, pl.ds(at, rows), :]
    spread(ids, tiles, rel_emb, full, slots)
    ones = jnp.ones((8, tiles.shape[2]), F32)
    lane = lax.broadcasted_iota(jnp.int32, (1, o0.shape[1]), 1)
    for s, out in enumerate((o0, o1, o2, o3)):
        out[0 : 2 * rows, :] = slots[2 * s : 2 * s + 2].reshape(2 * rows, -1)
        out[2 * rows :, :] = jnp.full((8, out.shape[1]), -1.0, F32)
    for b in range(2):
        sums = product(ones, tiles[b], ((1,), (1,)))
        for j in range(2):
            k = 2 * b + j
            line = jnp.where(lane == rows, ids[k].astype(F32), ids[4 + k].astype(F32))
            for out in (o0, o1, o2, o3):
                out[2 * rows + k : 2 * rows + k + 1, :] = line
                out[2 * rows + k : 2 * rows + k + 1, 0:rows] = sums[0:1, j * rows : (j + 1) * rows]


def pack_ring(place, p0, p1, p2, p3, out):
    rows = out.shape[1]
    for s, piece in enumerate((p0, p1, p2, p3)):
        out[s] = piece[0:rows, :]


def spread_next(place, ids, tiles, rel_emb, p0, p1, p2, p3, other, o0, o1, o2, o3, full, slots):
    z, c = place[0], place[1]
    rows = tiles.shape[1] // 2
    for s, piece in enumerate((p0, p1, p2, p3)):
        from_z = behind(z, s)
        for b in range(2):
            part = slice(b * rows, (b + 1) * rows)
            full[b, pl.ds(row(from_z * 2 + c, rows), rows), :] = piece[part, :]
            full[b, pl.ds(row(from_z * 2 + 1 - c, rows), rows), :] = other[s, part, :]
    spread(ids, tiles, rel_emb, full, slots)
    for s, out in enumerate((o0, o1, o2, o3)):
        out[...] = slots[2 * s : 2 * s + 2].reshape(2 * rows, -1)


def gates(place, state, w_self, w_gate, b_gate, update, self_part):
    held = state[...]
    update[...] = jax.nn.sigmoid(product(held, w_gate[...]) + b_gate[...])
    self_part[...] = product(held, w_self[...])


def advance(place, a0, a1, a2, a3, state, update, self_part, w_neigh, new, agg, candidate):
    rows = state.shape[0]
    total = (a0[0:rows, :] + a1[0:rows, :]) + (a2[0:rows, :] + a3[0:rows, :])
    agg[...] = total
    cand = jnp.tanh(product(total, w_neigh[...]) + self_part[...])
    candidate[...] = cand
    gate = update[...]
    new[...] = gate * cand + (1.0 - gate) * state[...]


def advance_with(place, a0, a1, a2, a3, state, update, self_part, w_neigh, c1, c2, c3, new, agg, candidate, n1, n2, n3):
    advance(place, a0, a1, a2, a3, state, update, self_part, w_neigh, new, agg, candidate)
    rows = new.shape[0]
    for piece, out in ((c1, n1), (c2, n2), (c3, n3)):
        out[0:rows, :] = new[...]
        out[rows:, :] = piece[...].reshape(rows, -1)


def retreat_math(d_new, state, update, candidate, w_neigh, d_pre, d_gate, d_agg, d_keep):
    gate, cand = update[...], candidate[...]
    rest = 1.0 - gate
    pre = d_new * gate * (1.0 - cand * cand)
    d_pre[...] = pre
    d_gate[...] = d_new * (cand - state[...]) * gate * rest
    d_agg[...] = product(pre, w_neigh[...], ((1,), (1,))).reshape(d_agg.shape)
    if d_keep is not None:
        d_keep[...] = d_new * rest


def retreat_last(place, cot, state, update, candidate, w_neigh, d_pre, d_gate, d_agg, d_keep):
    d_new = cot[...].reshape(state.shape)
    retreat_math(d_new, state, update, candidate, w_neigh, d_pre, d_gate, d_agg, d_keep)


def retreat(place, d0, d1, d2, d3, d_prev, cot, state, update, candidate, w_neigh, d_pre, d_gate, d_agg, d_keep):
    came = ((d0[0:2] + d1[0:2]) + (d2[0:2] + d3[0:2]) + cot[...]).reshape(state.shape)
    retreat_math(came + d_prev[...], state, update, candidate, w_neigh, d_pre, d_gate, d_agg, d_keep)


def before(place, d_keep, d_pre, d_gate, w_self, w_gate, d_prev):
    d_prev[...] = (
        d_keep[...]
        + product(d_pre[...], w_self[...], ((1,), (1,)))
        + product(d_gate[...], w_gate[...], ((1,), (1,)))
    )


def gather_back(place, ids, tiles, g0, g1, g2, g3, other, mine, rel_rows, held, res, full):
    z, c = place[0], place[1]
    rows = g0.shape[1]
    for s, piece in enumerate((g0, g1, g2, g3)):
        held[2 * s : 2 * s + 2] = piece[...]

    def step(b, carry):
        block = tiles[b]
        sums = jnp.sum(block, axis=1, keepdims=True)
        for j in range(2):
            value = held[ids[2 * b + j]]
            res[j * rows : (j + 1) * rows, :] = value
            total = jnp.sum(sums[j * rows : (j + 1) * rows] * value, axis=0, keepdims=True)
            rel_rows[2 * b + j] = jnp.broadcast_to(total, rel_rows.shape[1:])
        full[...] = product(block, res[...], ((0,), (0,)))
        for s in range(4):
            to = ahead(z, s)
            mine[s, b] = full[pl.ds(row(to * 2 + c, rows), rows), :]
            other[s, b] = full[pl.ds(row(to * 2 + 1 - c, rows), rows), :]
        return carry

    lax.fori_loop(0, 2, step, 0)


def gather_back_with(place, ids, tiles, g0, g1, g2, g3, s0, s1, s2, s3, other, mine, rel_rows, states, held, res, full):
    c = place[1]
    gather_back(place, ids, tiles, g0, g1, g2, g3, other, mine, rel_rows, held, res, full)
    for s, piece in enumerate((s0, s1, s2, s3)):
        states[s] = piece[2 + c]
        other[4 + s // 2, s % 2] = piece[2 + 1 - c]


def add_pairs(place, mine, got, n0, n1, n2, n3):
    for s, out in enumerate((n0, n1, n2, n3)):
        out[...] = mine[s] + got[s]


def add_pairs_with(place, mine, got, s0, s1, s2, s3, n0, n1, n2, n3):
    for s, (piece, out) in enumerate(((s0, n0), (s1, n1), (s2, n2), (s3, n3))):
        out[0:2] = mine[s] + got[s]
        out[2:4] = piece[...]


def cut_rows(place, own, got, *outs):
    z, c = place[0], place[1]
    rows, width = own.shape[0] // 8, own.shape[1]
    for s in range(4):
        to = ahead(z, s)
        outs[s][c] = own[pl.ds(row(to * 2 + c, rows), rows), :]
        outs[s][1 - c, 0 : rows // 2] = got[to, 2 * rows + 8 :, 0:width]
        outs[s][1 - c, rows // 2 :] = got[to, 2 * rows + 8 :, width:]


def join_rows(place, p0, p1, p2, p3, *refs):
    outs, stack = refs[:4], refs[4]
    z = place[0]
    rows = outs[0].shape[1]
    stack[z] = p0[...]
    for s, piece in enumerate((p1, p2, p3)):
        for core in range(2):
            stack[behind(z, s + 1), core] = piece[(2 + core) * rows : (3 + core) * rows, :]
    for t in range(4):
        for b in range(2):
            outs[t][b] = stack[(t // 2) * 2 + b, t % 2]


def cut_states(place, n0, n1, n2, n3, *refs):
    outs, stack = refs[:4], refs[4]
    z = place[0]
    rows = outs[0].shape[1]
    for t, state in enumerate((n0, n1, n2, n3)):
        for b in range(2):
            stack[(t // 2) * 2 + b, t % 2] = state[b * rows : (b + 1) * rows, :]
    for s in range(4):
        outs[s][...] = stack[ahead(z, s)]


def join_states(place, mine, got, out):
    z, c = place[0], place[1]
    rows = mine.shape[1]
    for s in range(4):
        from_z = behind(z, s)
        out[pl.ds(row(from_z * 2 + c, rows), rows), :] = mine[s]
        out[pl.ds(row(from_z * 2 + 1 - c, rows), rows), :] = got[4 + s // 2, s % 2]


def dense_grads(state, agg, pre, gate_in):
    pairs = ((agg, pre), (state, pre), (state, gate_in))
    return [product(a, b, ((0,), (0,))) for a, b in pairs], jnp.sum(gate_in, axis=0, keepdims=True)


def later_grads(count, place, *refs):
    tables, refs = refs[:count], refs[count:]
    lines, outs, stack = refs[4 * count : 5 * count], refs[5 * count : 5 * count + 5], refs[-1]
    for kind in range(4):
        for i in range(count):
            stack[kind, i] = refs[kind * count + i][...]
    for out in outs:
        out[...] = jnp.zeros_like(out)

    def step(i, carry):
        total, bias = dense_grads(stack[0, i], stack[1, i], stack[2, i], stack[3, i])
        for out, value in zip(outs[1:4], total):
            out[...] += value
        outs[4][...] += jnp.broadcast_to(bias, outs[4].shape)
        return carry

    lax.fori_loop(0, count, step, 0)
    for ids, line in zip(tables, lines):
        for k in range(4):
            outs[0][pl.ds(ids[4 + k], 1), :] += line[k, 0:1, :]


def weight_grads(place, state, agg, pre, gate_in, d_agg, l0, l1, l2, l3, *refs):
    later, d_bias, keep, give = refs[:4], refs[4], refs[5], refs[6]
    c = place[1]
    rows, width = d_agg.shape[1:]
    total, bias = dense_grads(state[...], agg[...], pre[...], gate_in[...])
    d_rel = later[0][...]
    relation = lax.broadcasted_iota(jnp.int32, (8, width), 1).astype(F32)
    for s, piece in enumerate((l0, l1, l2, l3)):
        line = piece[2 * rows :, 0:128]
        slot, rel, sums = line[:, rows : rows + 1], line[:, rows + 1 : rows + 2], line[:, 0:rows]
        found = sum(
            product(jnp.where(slot == float(2 * s + b), sums, 0.0), d_agg[b]) for b in range(2)
        )
        d_rel = d_rel + product((rel == relation).astype(F32), found, ((0,), (0,)))
    total = [d_rel] + [a + b[...] for a, b in zip(total, later[1:])]
    bias = bias + d_bias[0:1, :]
    parts = keep.shape[0]
    chunk = 2 * width // parts
    for out, own_half in ((keep, c == 0), (give, c != 0)):
        for i in range(2):
            value = jnp.where(own_half, total[i], total[2 + i])
            out[i * parts // 2 : (i + 1) * parts // 2, 0:chunk, :] = value.reshape(parts // 2, chunk, width)
        out[:, chunk:, :] = jnp.zeros((parts, out.shape[1] - chunk, width), F32)
        out[0, chunk : chunk + 1, :] = bias


def on_device(
    init_state, tiles, dst_block, rel_id, cotangent, rel_emb, w_neigh, w_self, w_gate, b_gate
):
    z, c, y, zl = lax.axis_index(Z), lax.axis_index("c"), lax.axis_index("y"), lax.axis_index("zl")
    snaps = 4
    tile, width = init_state.shape[1:]
    rows = tile // 8
    bias_row = b_gate.reshape(1, width)
    pair = (2, rows, width)
    flat = (2 * rows, width)

    own_tiles, own_cot, init = tiles[0, 0], cotangent[0, 0], init_state[0]
    here = jnp.stack([z, c, zl, y]).astype(jnp.int32)
    codes = (here, dst_block.reshape(2), rel_id.reshape(2))
    piece = (2 * rows + 8, tile)
    give, half = local(give_tiles, codes, (own_tiles, init, own_cot), [(4, piece[0] + rows // 2, tile), (tile // 2, width)])
    got_tiles = swap(give)
    held, ids = [None] * snaps, [None] * snaps
    part = [local(functools.partial(cut_tiles, core), codes, (own_tiles, got_tiles), [piece] * 4) for core in range(2)]
    ring = [part[0][0]] + [along(part[0][s], Z, s) for s in range(1, 4)]
    near = along(order(half, part[0][1]), "zl", 1)
    far = swap(near)
    cut_cot = local(cut_rows, (here,), (own_cot, got_tiles), [pair] * 4)
    ring, part[1], cut_cot = lax.optimization_barrier((ring, part[1], cut_cot))

    def join(core, ring):
        held[core], held[2 + core], ids[core], ids[2 + core] = local(
            join_tiles, (here,), ring, [(2, 2 * rows, tile)] * 2 + [8, 8]
        )

    join(0, ring)
    work = [(2, tile, width), (8, rows, width)]
    stored, states = [], []
    state = lines = carried = None
    for t in range(snaps):
        if t == 0:
            *to_y, state = local(
                spread_first,
                (here, ids[0]),
                (held[0], rel_emb, init, near, far),
                [(2 * rows + 8, width)] * 4 + [flat],
                work,
            )
        else:
            ring = [state] + [along(carried[s - 1] if carried else state, Z, s) for s in range(1, 4)]
            if carried:
                cots = local(join_rows, (here,), [cut_cot[0]] + ring[1:], [pair] * 4, [(4, 2, rows, width)])
                carried = None
            (packed,) = local(pack_ring, (here,), ring, [(4, *flat)])
            to_y = local(spread_next, (here, ids[t]), [held[t], rel_emb] + ring + [swap(packed)], [flat] * 4, work)
        came_y = [to_y[0]] + [along(to_y[s], "y", s) for s in range(1, 4)]
        if t == 0:
            lines = came_y
            late = [along(part[1][s], Z, s) for s in range(1, 4)]
            join(1, [part[1][0]] + late)
        update, self_part = local(gates, (here,), (state, w_self, w_gate, bias_row), [flat] * 2)
        terms = came_y + [state, update, self_part, w_neigh]
        if t == 1:
            new, agg, candidate, *carried = local(
                advance_with, (here,), terms + list(cut_cot[1:]), [flat] * 3 + [(4 * rows, width)] * 3
            )
        else:
            new, agg, candidate = local(advance, (here,), terms, [flat] * 3)
        stored.append((state, agg, update, candidate))
        states.append(new)
        state = new

    cut = local(cut_states, (here,), states, [pair] * 4, [(4, 2, rows, width)])

    d_prev = d_in = None
    pres, gates_in, rel_lines = [None] * snaps, [None] * snaps, []
    for t in reversed(range(snaps)):
        held_state, agg, update, candidate = stored[t]
        tail = (cots[t], held_state, update, candidate, w_neigh)
        outs = [flat, flat, pair, flat]
        if d_in is None:
            d_pre, d_gate, d_agg, d_keep = local(retreat_last, (here,), tail, outs)
        else:
            d_pre, d_gate, d_agg, d_keep = local(retreat, (here,), (*d_in, d_prev, *tail), outs)
        pres[t], gates_in[t] = d_pre, d_gate
        if t == 0:
            break
        pieces = [d_agg] + [along(d_agg, "y", -s) for s in range(1, 4)]
        (d_prev,) = local(before, (here,), (d_keep, d_pre, d_gate, w_self, w_gate), [flat])
        second = t == snaps - 2
        other, mine_rows, rel_rows, *mine_states = local(
            gather_back_with if second else gather_back,
            (here, ids[t]),
            [held[t]] + pieces + (list(d_in) if second else []),
            [(6 if second else 4, *pair), (4, *pair), (4, 8, width)] + [(4, rows, width)] * second,
            [(8, rows, width), flat, (tile, width)],
        )
        got = swap(other)
        if second:
            (state_out,) = local(join_states, (here,), (*mine_states, got), [(tile, width)])
        rel_lines.append(rel_rows)
        if t == 1:
            square = (width, width)
            later = local(
                functools.partial(later_grads, snaps - 1),
                (here, *ids[1:]),
                [s[0] for s in stored[1:]]
                + [s[1] for s in stored[1:]]
                + pres[1:]
                + gates_in[1:]
                + rel_lines[::-1],
                [square] * 4 + [(8, width)],
                [(4, snaps - 1, *flat)],
                flops=20_000_000_000,
            )
        if t == snaps - 1:
            parts = local(add_pairs_with, (here,), [mine_rows, got] + list(cut), [(4, rows, width)] * 4)
        else:
            parts = local(add_pairs, (here,), (mine_rows, got), [pair] * 4)
        d_in = [parts[0]] + [along(parts[s], Z, s) for s in range(1, 4)]

    parts = 16
    chunk = 2 * width // parts
    size = (parts, chunk + 8, width)
    keep, give = local(
        weight_grads, (here,), (stored[0][0], stored[0][1], d_pre, d_gate, d_agg, *lines, *later), [size] * 2
    )
    plane = ("zh", "zl", "y")
    summed = jnp.sum(lax.all_to_all(keep + swap(give), plane, 0, 0, tiled=True), axis=0)
    summed = (summed + along(summed, "b", 2)) + (along(summed, "b", 1) + along(summed, "b", 3))
    mine_sum = lax.all_to_all(jnp.broadcast_to(summed[None], size), plane, 0, 0, tiled=True)
    other_sum = swap(mine_sum)
    halves = (jnp.where(c == 0, mine_sum, other_sum), jnp.where(c == 0, other_sum, mine_sum))
    grads = [h[:, :chunk].reshape(2, width, width)[i] for h in halves for i in range(2)]
    return (state_out.reshape(1, 1, tile, width), *grads, mine_sum[0, chunk])


def solution(mesh):
    torus = Mesh(mesh.devices.reshape(2, 2, 4, 2, mesh.shape["batch"]), AXES)
    return jax.shard_map(
        on_device,
        mesh=torus,
        in_specs=(
            P("b", ENT, None),
            P("b", TM, ENT, None, None),
            P("b", TM, ENT),
            P("b", TM, ENT),
            P("b", TM, ENT, None),
            P(),
            P(),
            P(),
            P(),
            P(),
        ),
        out_specs=(P("b", TM, ENT, None), P(), P(), P(), P(), P()),
        check_vma=False,
    )
```

```python
import functools
import math

import jax
import jax.numpy as jnp
from jax import lax
from jax.experimental import pallas as pl
from jax.experimental.pallas import tpu as pltpu
from jax.sharding import Mesh
from jax.sharding import PartitionSpec as P


INTERPRET = False
VMEM_LIMIT = 16 * 1024 * 1024

AXES = ("zh", "c", "y", "zl", "b")
TM = ("zh", "c")
ENT = ("y", "zl")
Z = ("zh", "zl")
F32 = jnp.float32
BF16 = jnp.bfloat16


def halves(value):
    high = value.astype(BF16)
    return high, (value - high.astype(F32)).astype(BF16)


def product(left, right, dims=((1,), (0,))):
    (a, b), (c, d) = halves(left), halves(right)
    dot = lambda p, q: lax.dot_general(p, q, (dims, ((), ())), preferred_element_type=F32)
    return dot(a, c) + (dot(a, d) + dot(b, c))


def along(value, axis, steps):
    count = lax.axis_size(axis)
    return lax.ppermute(value, axis, [(i, (i + steps) % count) for i in range(count)])


def swap(value):
    return along(value, "c", 1)


def order(value, after):
    return lax.optimization_barrier((value, after))[0]


def local(kernel, tables, arrays, outs, scratch=(), flops=1_000_000):
    vmem, smem = pl.BlockSpec(memory_space=pltpu.VMEM), pl.BlockSpec(memory_space=pltpu.SMEM)
    size = sum(a.size for a in arrays) + sum(math.prod(o) for o in outs if not isinstance(o, int))
    return pl.pallas_call(
        kernel,
        out_shape=[
            jax.ShapeDtypeStruct((o,), jnp.int32) if isinstance(o, int) else jax.ShapeDtypeStruct(o, F32)
            for o in outs
        ],
        in_specs=[smem] * len(tables) + [vmem] * len(arrays),
        out_specs=[smem if isinstance(o, int) else vmem for o in outs],
        scratch_shapes=[pltpu.VMEM(s, F32) for s in scratch],
        cost_estimate=pl.CostEstimate(flops=flops, bytes_accessed=4 * size, transcendentals=0),
        compiler_params=pltpu.CompilerParams(vmem_limit_bytes=VMEM_LIMIT),
        interpret=INTERPRET,
    )(*tables, *arrays)


def ahead(z, s):
    return lax.rem(z + s, 4)


def behind(z, s):
    return lax.rem(z + 4 - s, 4)


def row(i, step):
    return pl.multiple_of(i * step, step)


def give_tiles(place, dst, rel, own, init, cot, out, half):
    c = place[1]
    rows = own.shape[1] // 8
    lane = lax.broadcasted_iota(jnp.int32, (8, own.shape[2]), 1) // 128
    codes = jnp.zeros(lane.shape, F32)
    for j in range(2):
        codes = jnp.where(lane == 2 * j, dst[j].astype(F32), codes)
        codes = jnp.where(lane == 2 * j + 1, rel[j].astype(F32), codes)
    for to in range(4):
        for j in range(2):
            out[to, j * rows : (j + 1) * rows, :] = own[j, pl.ds(row(to * 2 + 1 - c, rows), rows), :]
        out[to, 2 * rows : 2 * rows + 8, :] = codes
        lines = cot[pl.ds(row(to * 2 + 1 - c, rows), rows), :]
        out[to, 2 * rows + 8 :, 0 : cot.shape[1]] = lines[0 : rows // 2]
        out[to, 2 * rows + 8 :, cot.shape[1] :] = lines[rows // 2 :]
    half[...] = init[pl.ds(row(c, half.shape[0]), half.shape[0]), :]


def cut_tiles(core, place, dst, rel, own, got, *outs):
    z, c = place[0], place[1]
    rows = own.shape[1] // 8
    lane = lax.broadcasted_iota(jnp.int32, (8, own.shape[2]), 1) // 128

    @pl.when(c == core)
    def _():
        codes = jnp.zeros(lane.shape, F32)
        for j in range(2):
            codes = jnp.where(lane == 2 * j, dst[j].astype(F32), codes)
            codes = jnp.where(lane == 2 * j + 1, rel[j].astype(F32), codes)
        for s in range(4):
            to = ahead(z, s)
            for j in range(2):
                outs[s][j * rows : (j + 1) * rows, :] = own[j, pl.ds(row(to * 2 + c, rows), rows), :]
            outs[s][2 * rows :, :] = codes

    @pl.when(c != core)
    def _():
        for s in range(4):
            outs[s][...] = got[ahead(z, s), 0 : 2 * rows + 8, :]


def join_tiles(place, p0, p1, p2, p3, early, late, early_ids, late_ids):
    z, y = place[0], place[3]
    rows = early.shape[1]
    pieces = (p0, p1, p2, p3)
    codes = [
        [jnp.max(piece[rows : rows + 8, q * 128 : (q + 1) * 128]).astype(jnp.int32) for q in range(4)] for piece in pieces
    ]
    for s, piece in enumerate(pieces):
        from_z = behind(z, s)
        b = lax.rem(from_z, 2)

        def write(tiles, ids):
            tiles[b] = piece[0:rows, :]
            for j in range(2):
                dst, rel = codes[s][2 * j], codes[s][2 * j + 1]
                ids[2 * b + j] = lax.rem(lax.div(dst, 2) + 4 - y, 4) * 2 + lax.rem(dst, 2)
                ids[4 + 2 * b + j] = rel

        pl.when(from_z < 2)(functools.partial(write, early, early_ids))
        pl.when(from_z >= 2)(functools.partial(write, late, late_ids))


def spread(ids, tiles, rel_emb, full, slots):
    rows = tiles.shape[1] // 2
    slots[...] = jnp.zeros_like(slots)

    def step(b, carry):
        block = tiles[b]
        part = product(block, full[b])
        sums = jnp.sum(block, axis=1, keepdims=True)
        for j in range(2):
            line = rel_emb[pl.ds(ids[4 + 2 * b + j], 1), :]
            slots[ids[2 * b + j]] += part[j * rows : (j + 1) * rows] + sums[j * rows : (j + 1) * rows] * line
        return carry

    lax.fori_loop(0, 2, step, 0)


def spread_first(place, ids, tiles, rel_emb, init, near, far, o0, o1, o2, o3, own, full, slots):
    z, c, zl = place[0], place[1], place[2]
    half = near.shape[0]
    rows = tiles.shape[1] // 2
    full[zl] = init[...]
    full[1 - zl, pl.ds(row(c, half), half), :] = near[...]
    full[1 - zl, pl.ds(row(1 - c, half), half), :] = far[...]
    at = row(z * 2 + c, rows)
    for b in range(2):
        own[b * rows : (b + 1) * rows, :] = full[b, pl.ds(at, rows), :]
    spread(ids, tiles, rel_emb, full, slots)
    ones = jnp.ones((8, tiles.shape[2]), F32)
    lane = lax.broadcasted_iota(jnp.int32, (1, o0.shape[1]), 1)
    for s, out in enumerate((o0, o1, o2, o3)):
        out[0 : 2 * rows, :] = slots[2 * s : 2 * s + 2].reshape(2 * rows, -1)
        out[2 * rows :, :] = jnp.full((8, out.shape[1]), -1.0, F32)
    for b in range(2):
        sums = product(ones, tiles[b], ((1,), (1,)))
        for j in range(2):
            k = 2 * b + j
            line = jnp.where(lane == rows, ids[k].astype(F32), ids[4 + k].astype(F32))
            for out in (o0, o1, o2, o3):
                out[2 * rows + k : 2 * rows + k + 1, :] = line
                out[2 * rows + k : 2 * rows + k + 1, 0:rows] = sums[0:1, j * rows : (j + 1) * rows]


def pack_ring(place, p0, p1, p2, p3, out):
    rows = out.shape[1]
    for s, piece in enumerate((p0, p1, p2, p3)):
        out[s] = piece[0:rows, :]


def spread_next(place, ids, tiles, rel_emb, p0, p1, p2, p3, other, o0, o1, o2, o3, full, slots):
    z, c = place[0], place[1]
    rows = tiles.shape[1] // 2
    for s, piece in enumerate((p0, p1, p2, p3)):
        from_z = behind(z, s)
        for b in range(2):
            part = slice(b * rows, (b + 1) * rows)
            full[b, pl.ds(row(from_z * 2 + c, rows), rows), :] = piece[part, :]
            full[b, pl.ds(row(from_z * 2 + 1 - c, rows), rows), :] = other[s, part, :]
    spread(ids, tiles, rel_emb, full, slots)
    for s, out in enumerate((o0, o1, o2, o3)):
        out[...] = slots[2 * s : 2 * s + 2].reshape(2 * rows, -1)


def gates(place, state, w_self, w_gate, b_gate, update, self_part):
    held = state[...]
    update[...] = jax.nn.sigmoid(product(held, w_gate[...]) + b_gate[...])
    self_part[...] = product(held, w_self[...])


def advance(place, a0, a1, a2, a3, state, update, self_part, w_neigh, new, agg, candidate):
    rows = state.shape[0]
    total = (a0[0:rows, :] + a1[0:rows, :]) + (a2[0:rows, :] + a3[0:rows, :])
    agg[...] = total
    cand = jnp.tanh(product(total, w_neigh[...]) + self_part[...])
    candidate[...] = cand
    gate = update[...]
    new[...] = gate * cand + (1.0 - gate) * state[...]


def retreat_math(d_new, state, update, candidate, w_neigh, d_pre, d_gate, d_agg, d_keep):
    gate, cand = update[...], candidate[...]
    rest = 1.0 - gate
    pre = d_new * gate * (1.0 - cand * cand)
    d_pre[...] = pre
    d_gate[...] = d_new * (cand - state[...]) * gate * rest
    d_agg[...] = product(pre, w_neigh[...], ((1,), (1,))).reshape(d_agg.shape)
    if d_keep is not None:
        d_keep[...] = d_new * rest


def retreat_last(place, cot, state, update, candidate, w_neigh, d_pre, d_gate, d_agg, d_keep):
    d_new = cot[...].reshape(state.shape)
    retreat_math(d_new, state, update, candidate, w_neigh, d_pre, d_gate, d_agg, d_keep)


def retreat(place, d0, d1, d2, d3, d_prev, cot, state, update, candidate, w_neigh, d_pre, d_gate, d_agg, d_keep):
    came = ((d0[0:2] + d1[0:2]) + (d2[0:2] + d3[0:2]) + cot[...]).reshape(state.shape)
    retreat_math(came + d_prev[...], state, update, candidate, w_neigh, d_pre, d_gate, d_agg, d_keep)


def before(place, d_keep, d_pre, d_gate, w_self, w_gate, d_prev):
    d_prev[...] = (
        d_keep[...]
        + product(d_pre[...], w_self[...], ((1,), (1,)))
        + product(d_gate[...], w_gate[...], ((1,), (1,)))
    )


def gather_back(place, ids, tiles, g0, g1, g2, g3, other, mine, rel_rows, held, res, full):
    z, c = place[0], place[1]
    rows = g0.shape[1]
    for s, piece in enumerate((g0, g1, g2, g3)):
        held[2 * s : 2 * s + 2] = piece[...]

    def step(b, carry):
        block = tiles[b]
        sums = jnp.sum(block, axis=1, keepdims=True)
        for j in range(2):
            value = held[ids[2 * b + j]]
            res[j * rows : (j + 1) * rows, :] = value
            total = jnp.sum(sums[j * rows : (j + 1) * rows] * value, axis=0, keepdims=True)
            rel_rows[2 * b + j] = jnp.broadcast_to(total, rel_rows.shape[1:])
        full[...] = product(block, res[...], ((0,), (0,)))
        for s in range(4):
            to = ahead(z, s)
            mine[s, b] = full[pl.ds(row(to * 2 + c, rows), rows), :]
            other[s, b] = full[pl.ds(row(to * 2 + 1 - c, rows), rows), :]
        return carry

    lax.fori_loop(0, 2, step, 0)


def gather_back_with(place, ids, tiles, g0, g1, g2, g3, s0, s1, s2, s3, other, mine, rel_rows, states, held, res, full):
    c = place[1]
    gather_back(place, ids, tiles, g0, g1, g2, g3, other, mine, rel_rows, held, res, full)
    for s, piece in enumerate((s0, s1, s2, s3)):
        states[s] = piece[c]
        other[4 + s // 2, s % 2] = piece[1 - c]


def add_pairs(place, mine, got, n0, n1, n2, n3):
    for s, out in enumerate((n0, n1, n2, n3)):
        out[...] = mine[s] + got[s]


def cut_rows(place, own, got, *outs):
    z, c = place[0], place[1]
    rows, width = own.shape[0] // 8, own.shape[1]
    for s in range(4):
        to = ahead(z, s)
        outs[s][c] = own[pl.ds(row(to * 2 + c, rows), rows), :]
        outs[s][1 - c, 0 : rows // 2] = got[to, 2 * rows + 8 :, 0:width]
        outs[s][1 - c, rows // 2 :] = got[to, 2 * rows + 8 :, width:]


def join_rows(place, p0, p1, p2, p3, *refs):
    outs, stack = refs[:4], refs[4]
    z = place[0]
    for s, piece in enumerate((p0, p1, p2, p3)):
        stack[behind(z, s)] = piece[...]
    for t in range(4):
        for b in range(2):
            outs[t][b] = stack[(t // 2) * 2 + b, t % 2]


def cut_states(place, n0, n1, n2, n3, *refs):
    outs, stack = refs[:4], refs[4]
    z = place[0]
    rows = outs[0].shape[1]
    for t, state in enumerate((n0, n1, n2, n3)):
        for b in range(2):
            stack[(t // 2) * 2 + b, t % 2] = state[b * rows : (b + 1) * rows, :]
    for s in range(4):
        outs[s][...] = stack[ahead(z, s)]


def join_states(place, mine, got, out):
    z, c = place[0], place[1]
    rows = mine.shape[1]
    for s in range(4):
        from_z = behind(z, s)
        out[pl.ds(row(from_z * 2 + c, rows), rows), :] = mine[s]
        out[pl.ds(row(from_z * 2 + 1 - c, rows), rows), :] = got[4 + s // 2, s % 2]


def dense_grads(state, agg, pre, gate_in):
    pairs = ((agg, pre), (state, pre), (state, gate_in))
    return [product(a, b, ((0,), (0,))) for a, b in pairs], jnp.sum(gate_in, axis=0, keepdims=True)


def later_grads(count, place, *refs):
    tables, refs = refs[:count], refs[count:]
    lines, outs, stack = refs[4 * count : 5 * count], refs[5 * count : 5 * count + 5], refs[-1]
    for kind in range(4):
        for i in range(count):
            stack[kind, i] = refs[kind * count + i][...]
    for out in outs:
        out[...] = jnp.zeros_like(out)

    def step(i, carry):
        total, bias = dense_grads(stack[0, i], stack[1, i], stack[2, i], stack[3, i])
        for out, value in zip(outs[1:4], total):
            out[...] += value
        outs[4][...] += jnp.broadcast_to(bias, outs[4].shape)
        return carry

    lax.fori_loop(0, count, step, 0)
    for ids, line in zip(tables, lines):
        for k in range(4):
            outs[0][pl.ds(ids[4 + k], 1), :] += line[k, 0:1, :]


def weight_grads(place, state, agg, pre, gate_in, d_agg, l0, l1, l2, l3, *refs):
    later, d_bias, keep, give = refs[:4], refs[4], refs[5], refs[6]
    c = place[1]
    rows, width = d_agg.shape[1:]
    total, bias = dense_grads(state[...], agg[...], pre[...], gate_in[...])
    d_rel = later[0][...]
    relation = lax.broadcasted_iota(jnp.int32, (8, width), 1).astype(F32)
    for s, piece in enumerate((l0, l1, l2, l3)):
        line = piece[2 * rows :, 0:128]
        slot, rel, sums = line[:, rows : rows + 1], line[:, rows + 1 : rows + 2], line[:, 0:rows]
        found = sum(
            product(jnp.where(slot == float(2 * s + b), sums, 0.0), d_agg[b]) for b in range(2)
        )
        d_rel = d_rel + product((rel == relation).astype(F32), found, ((0,), (0,)))
    total = [d_rel] + [a + b[...] for a, b in zip(total, later[1:])]
    bias = bias + d_bias[0:1, :]
    parts = keep.shape[0]
    chunk = 2 * width // parts
    for out, own_half in ((keep, c == 0), (give, c != 0)):
        for i in range(2):
            value = jnp.where(own_half, total[i], total[2 + i])
            out[i * parts // 2 : (i + 1) * parts // 2, 0:chunk, :] = value.reshape(parts // 2, chunk, width)
        out[:, chunk:, :] = jnp.zeros((parts, out.shape[1] - chunk, width), F32)
        out[0, chunk : chunk + 1, :] = bias


def on_device(
    init_state, tiles, dst_block, rel_id, cotangent, rel_emb, w_neigh, w_self, w_gate, b_gate
):
    z, c, y, zl = lax.axis_index(Z), lax.axis_index("c"), lax.axis_index("y"), lax.axis_index("zl")
    snaps = 4
    tile, width = init_state.shape[1:]
    rows = tile // 8
    bias_row = b_gate.reshape(1, width)
    pair = (2, rows, width)
    flat = (2 * rows, width)

    own_tiles, own_cot, init = tiles[0, 0], cotangent[0, 0], init_state[0]
    here = jnp.stack([z, c, zl, y]).astype(jnp.int32)
    codes = (here, dst_block.reshape(2), rel_id.reshape(2))
    piece = (2 * rows + 8, tile)
    give, half = local(give_tiles, codes, (own_tiles, init, own_cot), [(4, piece[0] + rows // 2, tile), (tile // 2, width)])
    got_tiles = swap(give)
    held, ids = [None] * snaps, [None] * snaps
    part = [local(functools.partial(cut_tiles, core), codes, (own_tiles, got_tiles), [piece] * 4) for core in range(2)]
    ring = [part[0][0]] + [along(part[0][s], Z, s) for s in range(1, 4)]
    near = along(order(half, part[0][1]), "zl", 1)
    far = swap(near)
    cut_cot = local(cut_rows, (here,), (own_cot, got_tiles), [pair] * 4)
    ring, part[1], cut_cot = lax.optimization_barrier((ring, part[1], cut_cot))

    def join(core, ring):
        held[core], held[2 + core], ids[core], ids[2 + core] = local(
            join_tiles, (here,), ring, [(2, 2 * rows, tile)] * 2 + [8, 8]
        )

    join(0, ring)
    work = [(2, tile, width), (8, rows, width)]
    stored, states = [], []
    state = lines = None
    for t in range(snaps):
        if t == 0:
            *to_y, state = local(
                spread_first,
                (here, ids[0]),
                (held[0], rel_emb, init, near, far),
                [(2 * rows + 8, width)] * 4 + [flat],
                work,
            )
        else:
            ring = [state] + [along(state, Z, s) for s in range(1, 4)]
            (packed,) = local(pack_ring, (here,), ring, [(4, *flat)])
            to_y = local(spread_next, (here, ids[t]), [held[t], rel_emb] + ring + [swap(packed)], [flat] * 4, work)
        came_y = [to_y[0]] + [along(to_y[s], "y", s) for s in range(1, 4)]
        if t == 0:
            lines = came_y
            late = [along(part[1][s], Z, s) for s in range(1, 4)]
            join(1, [part[1][0]] + late)
        update, self_part = local(gates, (here,), (state, w_self, w_gate, bias_row), [flat] * 2)
        terms = came_y + [state, update, self_part, w_neigh]
        if t == 1:
            ring = [cut_cot[0]] + [along(cut_cot[s], Z, s) for s in range(1, 4)]
            cots = local(join_rows, (here,), ring, [pair] * 4, [(4, 2, rows, width)])
        new, agg, candidate = local(advance, (here,), terms, [flat] * 3)
        stored.append((state, agg, update, candidate))
        states.append(new)
        state = new

    cut = local(cut_states, (here,), states, [pair] * 4, [(4, 2, rows, width)])
    cut = [cut[0]] + [along(cut[s], Z, s) for s in range(1, 4)]

    d_prev = d_in = None
    pres, gates_in, rel_lines = [None] * snaps, [None] * snaps, []
    for t in reversed(range(snaps)):
        held_state, agg, update, candidate = stored[t]
        tail = (cots[t], held_state, update, candidate, w_neigh)
        outs = [flat, flat, pair, flat]
        if d_in is None:
            d_pre, d_gate, d_agg, d_keep = local(retreat_last, (here,), tail, outs)
        else:
            d_pre, d_gate, d_agg, d_keep = local(retreat, (here,), (*d_in, d_prev, *tail), outs)
        pres[t], gates_in[t] = d_pre, d_gate
        if t == 0:
            break
        pieces = [d_agg] + [along(d_agg, "y", -s) for s in range(1, 4)]
        (d_prev,) = local(before, (here,), (d_keep, d_pre, d_gate, w_self, w_gate), [flat])
        second = t == snaps - 2
        other, mine_rows, rel_rows, *mine_states = local(
            gather_back_with if second else gather_back,
            (here, ids[t]),
            [held[t]] + pieces + (cut if second else []),
            [(6 if second else 4, *pair), (4, *pair), (4, 8, width)] + [(4, rows, width)] * second,
            [(8, rows, width), flat, (tile, width)],
        )
        got = swap(other)
        if second:
            (state_out,) = local(join_states, (here,), (*mine_states, got), [(tile, width)])
        rel_lines.append(rel_rows)
        if t == 1:
            square = (width, width)
            later = local(
                functools.partial(later_grads, snaps - 1),
                (here, *ids[1:]),
                [s[0] for s in stored[1:]]
                + [s[1] for s in stored[1:]]
                + pres[1:]
                + gates_in[1:]
                + rel_lines[::-1],
                [square] * 4 + [(8, width)],
                [(4, snaps - 1, *flat)],
                flops=20_000_000_000,
            )
        parts = local(add_pairs, (here,), (mine_rows, got), [pair] * 4)
        d_in = [parts[0]] + [along(parts[s], Z, s) for s in range(1, 4)]

    parts = 16
    chunk = 2 * width // parts
    size = (parts, chunk + 8, width)
    keep, give = local(
        weight_grads, (here,), (stored[0][0], stored[0][1], d_pre, d_gate, d_agg, *lines, *later), [size] * 2
    )
    plane = ("zh", "zl", "y")
    summed = jnp.sum(lax.all_to_all(keep + swap(give), plane, 0, 0, tiled=True), axis=0)
    summed = (summed + along(summed, "b", 2)) + (along(summed, "b", 1) + along(summed, "b", 3))
    mine_sum = lax.all_to_all(jnp.broadcast_to(summed[None], size), plane, 0, 0, tiled=True)
    other_sum = swap(mine_sum)
    halves = (jnp.where(c == 0, mine_sum, other_sum), jnp.where(c == 0, other_sum, mine_sum))
    grads = [h[:, :chunk].reshape(2, width, width)[i] for h in halves for i in range(2)]
    return (state_out.reshape(1, 1, tile, width), *grads, mine_sum[0, chunk])


def solution(mesh):
    torus = Mesh(mesh.devices.reshape(2, 2, 4, 2, mesh.shape["batch"]), AXES)
    return jax.shard_map(
        on_device,
        mesh=torus,
        in_specs=(
            P("b", ENT, None),
            P("b", TM, ENT, None, None),
            P("b", TM, ENT),
            P("b", TM, ENT),
            P("b", TM, ENT, None),
            P(),
            P(),
            P(),
            P(),
            P(),
        ),
        out_specs=(P("b", TM, ENT, None), P(), P(), P(), P(), P()),
        check_vma=False,
    )
```

```python
import functools
import math

import jax
import jax.numpy as jnp
from jax import lax
from jax.experimental import pallas as pl
from jax.experimental.pallas import tpu as pltpu
from jax.sharding import Mesh
from jax.sharding import PartitionSpec as P


INTERPRET = False
VMEM_LIMIT = 16 * 1024 * 1024

AXES = ("zh", "c", "y", "zl", "b")
TM = ("zh", "c")
ENT = ("y", "zl")
Z = ("zh", "zl")
F32 = jnp.float32
BF16 = jnp.bfloat16


def halves(value):
    high = value.astype(BF16)
    return high, (value - high.astype(F32)).astype(BF16)


def product(left, right, dims=((1,), (0,))):
    (a, b), (c, d) = halves(left), halves(right)
    dot = lambda p, q: lax.dot_general(p, q, (dims, ((), ())), preferred_element_type=F32)
    return dot(a, c) + (dot(a, d) + dot(b, c))


def along(value, axis, steps):
    count = lax.axis_size(axis)
    return lax.ppermute(value, axis, [(i, (i + steps) % count) for i in range(count)])


def swap(value):
    return along(value, "c", 1)


def local(kernel, tables, arrays, outs, scratch=(), flops=1_000_000, arrays_in=pltpu.VMEM, semaphores=()):
    vmem, smem = pl.BlockSpec(memory_space=pltpu.VMEM), pl.BlockSpec(memory_space=pltpu.SMEM)
    size = sum(a.size for a in arrays) + sum(math.prod(o) for o in outs if not isinstance(o, int))
    return pl.pallas_call(
        kernel,
        out_shape=[
            jax.ShapeDtypeStruct((o,), jnp.int32) if isinstance(o, int) else jax.ShapeDtypeStruct(o, F32)
            for o in outs
        ],
        in_specs=[smem] * len(tables) + [pl.BlockSpec(memory_space=arrays_in)] * len(arrays),
        out_specs=[smem if isinstance(o, int) else vmem for o in outs],
        scratch_shapes=[pltpu.VMEM(s, F32) for s in scratch] + list(semaphores),
        cost_estimate=pl.CostEstimate(flops=flops, bytes_accessed=4 * size, transcendentals=0),
        compiler_params=pltpu.CompilerParams(vmem_limit_bytes=VMEM_LIMIT),
        interpret=INTERPRET,
    )(*tables, *(a if arrays_in is pltpu.VMEM or INTERPRET else pltpu.with_memory_space_constraint(a, arrays_in) for a in arrays))


def ahead(z, s):
    return lax.rem(z + s, 4)


def behind(z, s):
    return lax.rem(z + 4 - s, 4)


def row(i, step):
    return pl.multiple_of(i * step, step)


def id_codes(place, lane):
    codes = jnp.zeros(lane.shape, F32)
    for j in range(2):
        codes = jnp.where(lane == 2 * j, place[4 + j].astype(F32), codes)
        codes = jnp.where(lane == 2 * j + 1, place[6 + j].astype(F32), codes)
    return codes


def give_tiles(place, own, init, cot, out, half0, half1, sems):
    c = place[1]
    rows, width = own.shape[1] // 8, init.shape[1]
    quarter = half0.shape[0]
    copies = []

    def copy(source, target):
        copies.append(pltpu.make_async_copy(source, target, sems.at[len(copies)]))
        copies[-1].start()

    for to in range(4):
        at = row(to * 2 + 1 - c, rows)
        for j in range(2):
            copy(own.at[j, pl.ds(at, rows), :], out.at[to, j * rows : (j + 1) * rows, :])
        for i in range(2):
            copy(
                cot.at[pl.ds(row(4 * to + 2 - 2 * c + i, rows // 2), rows // 2), :],
                out.at[to, 2 * rows + 8 :, i * width : (i + 1) * width],
            )
    copy(init.at[pl.ds(row(2 * c, quarter), quarter), :], half0)
    copy(init.at[pl.ds(row(2 * c + 1, quarter), quarter), :], half1)
    lane = lax.broadcasted_iota(jnp.int32, (8, own.shape[2]), 1) // 128
    codes = id_codes(place, lane)
    for to in range(4):
        out[to, 2 * rows : 2 * rows + 8, :] = codes
    for waited in copies:
        waited.wait()


def cut_tiles(core, place, own, got, *outs):
    z, c = place[0], place[1]
    rows = own.shape[1] // 8
    lane = lax.broadcasted_iota(jnp.int32, (8, own.shape[2]), 1) // 128

    @pl.when(c == core)
    def _():
        codes = id_codes(place, lane)
        for s in range(4):
            to = ahead(z, s)
            for j in range(2):
                outs[s][j * rows : (j + 1) * rows, :] = own[j, pl.ds(row(to * 2 + c, rows), rows), :]
            outs[s][2 * rows :, :] = codes

    @pl.when(c != core)
    def _():
        for s in range(4):
            outs[s][...] = got[ahead(z, s), 0 : 2 * rows + 8, :]


def join_tiles(place, p0, p1, p2, p3, early, late, early_ids, late_ids):
    z, y = place[0], place[3]
    rows = early.shape[1]
    pieces = (p0, p1, p2, p3)
    codes = [
        [jnp.max(piece[rows : rows + 8, q * 128 : (q + 1) * 128]).astype(jnp.int32) for q in range(4)] for piece in pieces
    ]
    for s, piece in enumerate(pieces):
        from_z = behind(z, s)
        b = lax.rem(from_z, 2)

        def write(tiles, ids):
            tiles[b] = piece[0:rows, :]
            for j in range(2):
                dst, rel = codes[s][2 * j], codes[s][2 * j + 1]
                ids[2 * b + j] = lax.rem(lax.div(dst, 2) + 4 - y, 4) * 2 + lax.rem(dst, 2)
                ids[4 + 2 * b + j] = rel

        pl.when(from_z < 2)(functools.partial(write, early, early_ids))
        pl.when(from_z >= 2)(functools.partial(write, late, late_ids))


def spread(ids, tiles, rel_emb, full, slots):
    rows = tiles.shape[1] // 2
    slots[...] = jnp.zeros_like(slots)

    def step(b, carry):
        block = tiles[b]
        part = product(block, full[b])
        sums = jnp.sum(block, axis=1, keepdims=True)
        for j in range(2):
            line = rel_emb[pl.ds(ids[4 + 2 * b + j], 1), :]
            slots[ids[2 * b + j]] += part[j * rows : (j + 1) * rows] + sums[j * rows : (j + 1) * rows] * line
        return carry

    lax.fori_loop(0, 2, step, 0)


def spread_first(place, ids, tiles, rel_emb, init, near0, near1, far0, far1, o0, o1, o2, o3, own, full, slots):
    z, c, zl = place[0], place[1], place[2]
    quarter = near0.shape[0]
    rows = tiles.shape[1] // 2
    full[zl] = init[...]
    for i, (near, far) in enumerate(((near0, far0), (near1, far1))):
        full[1 - zl, pl.ds(row(2 * c + i, quarter), quarter), :] = near[...]
        full[1 - zl, pl.ds(row(2 - 2 * c + i, quarter), quarter), :] = far[...]
    at = row(z * 2 + c, rows)
    for b in range(2):
        own[b * rows : (b + 1) * rows, :] = full[b, pl.ds(at, rows), :]
    spread(ids, tiles, rel_emb, full, slots)
    ones = jnp.ones((8, tiles.shape[2]), F32)
    lane = lax.broadcasted_iota(jnp.int32, (1, o0.shape[1]), 1)
    for s, out in enumerate((o0, o1, o2, o3)):
        out[0 : 2 * rows, :] = slots[2 * s : 2 * s + 2].reshape(2 * rows, -1)
        out[2 * rows :, :] = jnp.full((8, out.shape[1]), -1.0, F32)
    for b in range(2):
        sums = product(ones, tiles[b], ((1,), (1,)))
        for j in range(2):
            k = 2 * b + j
            line = jnp.where(lane == rows, ids[k].astype(F32), ids[4 + k].astype(F32))
            for out in (o0, o1, o2, o3):
                out[2 * rows + k : 2 * rows + k + 1, :] = line
                out[2 * rows + k : 2 * rows + k + 1, 0:rows] = sums[0:1, j * rows : (j + 1) * rows]


def pack_ring(place, p0, p1, p2, p3, out):
    rows = out.shape[1]
    for s, piece in enumerate((p0, p1, p2, p3)):
        out[s] = piece[0:rows, :]


def spread_next(place, ids, tiles, rel_emb, p0, p1, p2, p3, other, o0, o1, o2, o3, full, slots):
    z, c = place[0], place[1]
    rows = tiles.shape[1] // 2
    for s, piece in enumerate((p0, p1, p2, p3)):
        from_z = behind(z, s)
        for b in range(2):
            part = slice(b * rows, (b + 1) * rows)
            full[b, pl.ds(row(from_z * 2 + c, rows), rows), :] = piece[part, :]
            full[b, pl.ds(row(from_z * 2 + 1 - c, rows), rows), :] = other[s, part, :]
    spread(ids, tiles, rel_emb, full, slots)
    for s, out in enumerate((o0, o1, o2, o3)):
        out[...] = slots[2 * s : 2 * s + 2].reshape(2 * rows, -1)


def gates(place, state, w_self, w_gate, b_gate, update, self_part):
    held = state[...]
    update[...] = jax.nn.sigmoid(product(held, w_gate[...]) + b_gate[...])
    self_part[...] = product(held, w_self[...])


def advance(place, a0, a1, a2, a3, state, update, self_part, w_neigh, new, agg, candidate):
    rows = state.shape[0]
    total = (a0[0:rows, :] + a1[0:rows, :]) + (a2[0:rows, :] + a3[0:rows, :])
    agg[...] = total
    cand = jnp.tanh(product(total, w_neigh[...]) + self_part[...])
    candidate[...] = cand
    gate = update[...]
    new[...] = gate * cand + (1.0 - gate) * state[...]


def retreat_math(d_new, state, update, candidate, w_neigh, d_pre, d_gate, d_agg, d_keep):
    gate, cand = update[...], candidate[...]
    rest = 1.0 - gate
    pre = d_new * gate * (1.0 - cand * cand)
    d_pre[...] = pre
    d_gate[...] = d_new * (cand - state[...]) * gate * rest
    d_agg[...] = product(pre, w_neigh[...], ((1,), (1,))).reshape(d_agg.shape)
    if d_keep is not None:
        d_keep[...] = d_new * rest


def retreat_last(place, cot, state, update, candidate, w_neigh, d_pre, d_gate, d_agg, d_keep):
    d_new = cot[...].reshape(state.shape)
    retreat_math(d_new, state, update, candidate, w_neigh, d_pre, d_gate, d_agg, d_keep)


def retreat(place, d0, d1, d2, d3, d_prev, cot, state, update, candidate, w_neigh, d_pre, d_gate, d_agg, d_keep):
    came = ((d0[0:2] + d1[0:2]) + (d2[0:2] + d3[0:2]) + cot[...]).reshape(state.shape)
    retreat_math(came + d_prev[...], state, update, candidate, w_neigh, d_pre, d_gate, d_agg, d_keep)


def before(place, d_keep, d_pre, d_gate, w_self, w_gate, d_prev):
    d_prev[...] = (
        d_keep[...]
        + product(d_pre[...], w_self[...], ((1,), (1,)))
        + product(d_gate[...], w_gate[...], ((1,), (1,)))
    )


def gather_back(place, ids, tiles, g0, g1, g2, g3, other, mine, rel_rows, held, res, full):
    z, c = place[0], place[1]
    rows = g0.shape[1]
    for s, piece in enumerate((g0, g1, g2, g3)):
        held[2 * s : 2 * s + 2] = piece[...]

    def step(b, carry):
        block = tiles[b]
        sums = jnp.sum(block, axis=1, keepdims=True)
        for j in range(2):
            value = held[ids[2 * b + j]]
            res[j * rows : (j + 1) * rows, :] = value
            total = jnp.sum(sums[j * rows : (j + 1) * rows] * value, axis=0, keepdims=True)
            rel_rows[2 * b + j] = jnp.broadcast_to(total, rel_rows.shape[1:])
        full[...] = product(block, res[...], ((0,), (0,)))
        for s in range(4):
            to = ahead(z, s)
            mine[s, b] = full[pl.ds(row(to * 2 + c, rows), rows), :]
            other[s, b] = full[pl.ds(row(to * 2 + 1 - c, rows), rows), :]
        return carry

    lax.fori_loop(0, 2, step, 0)


def gather_back_with(place, ids, tiles, g0, g1, g2, g3, s0, s1, s2, s3, other, mine, rel_rows, states, held, res, full):
    c = place[1]
    gather_back(place, ids, tiles, g0, g1, g2, g3, other, mine, rel_rows, held, res, full)
    for s, piece in enumerate((s0, s1, s2, s3)):
        states[s] = piece[c]
        other[4 + s // 2, s % 2] = piece[1 - c]


def add_pairs(place, mine, got, n0, n1, n2, n3):
    for s, out in enumerate((n0, n1, n2, n3)):
        out[...] = mine[s] + got[s]


def cut_rows(place, own, got, *outs):
    z, c = place[0], place[1]
    rows, width = own.shape[0] // 8, own.shape[1]
    for s in range(4):
        to = ahead(z, s)
        outs[s][c] = own[pl.ds(row(to * 2 + c, rows), rows), :]
        outs[s][1 - c, 0 : rows // 2] = got[to, 2 * rows + 8 :, 0:width]
        outs[s][1 - c, rows // 2 :] = got[to, 2 * rows + 8 :, width:]


def join_rows(place, p0, p1, p2, p3, *refs):
    outs, stack = refs[:4], refs[4]
    z = place[0]
    for s, piece in enumerate((p0, p1, p2, p3)):
        stack[behind(z, s)] = piece[...]
    for t in range(4):
        for b in range(2):
            outs[t][b] = stack[(t // 2) * 2 + b, t % 2]


def cut_states(place, n0, n1, n2, n3, *refs):
    outs, stack = refs[:4], refs[4]
    z = place[0]
    rows = outs[0].shape[1]
    for t, state in enumerate((n0, n1, n2, n3)):
        for b in range(2):
            stack[(t // 2) * 2 + b, t % 2] = state[b * rows : (b + 1) * rows, :]
    for s in range(4):
        outs[s][...] = stack[ahead(z, s)]


def join_states(place, mine, got, out):
    z, c = place[0], place[1]
    rows = mine.shape[1]
    for s in range(4):
        from_z = behind(z, s)
        out[pl.ds(row(from_z * 2 + c, rows), rows), :] = mine[s]
        out[pl.ds(row(from_z * 2 + 1 - c, rows), rows), :] = got[4 + s // 2, s % 2]


def dense_grads(state, agg, pre, gate_in):
    pairs = ((agg, pre), (state, pre), (state, gate_in))
    return [product(a, b, ((0,), (0,))) for a, b in pairs], jnp.sum(gate_in, axis=0, keepdims=True)


def later_grads(count, place, *refs):
    tables, refs = refs[:count], refs[count:]
    lines, outs, stack = refs[4 * count : 5 * count], refs[5 * count : 5 * count + 5], refs[-1]
    for kind in range(4):
        for i in range(count):
            stack[kind, i] = refs[kind * count + i][...]
    for out in outs:
        out[...] = jnp.zeros_like(out)

    def step(i, carry):
        total, bias = dense_grads(stack[0, i], stack[1, i], stack[2, i], stack[3, i])
        for out, value in zip(outs[1:4], total):
            out[...] += value
        outs[4][...] += jnp.broadcast_to(bias, outs[4].shape)
        return carry

    lax.fori_loop(0, count, step, 0)
    for ids, line in zip(tables, lines):
        for k in range(4):
            outs[0][pl.ds(ids[4 + k], 1), :] += line[k, 0:1, :]


def weight_grads(place, state, agg, pre, gate_in, d_agg, l0, l1, l2, l3, *refs):
    later, d_bias, keep, give = refs[:4], refs[4], refs[5], refs[6]
    c = place[1]
    rows, width = d_agg.shape[1:]
    total, bias = dense_grads(state[...], agg[...], pre[...], gate_in[...])
    d_rel = later[0][...]
    relation = lax.broadcasted_iota(jnp.int32, (8, width), 1).astype(F32)
    for s, piece in enumerate((l0, l1, l2, l3)):
        line = piece[2 * rows :, 0:128]
        slot, rel, sums = line[:, rows : rows + 1], line[:, rows + 1 : rows + 2], line[:, 0:rows]
        found = sum(
            product(jnp.where(slot == float(2 * s + b), sums, 0.0), d_agg[b]) for b in range(2)
        )
        d_rel = d_rel + product((rel == relation).astype(F32), found, ((0,), (0,)))
    total = [d_rel] + [a + b[...] for a, b in zip(total, later[1:])]
    bias = bias + d_bias[0:1, :]
    parts = keep.shape[0]
    chunk = 2 * width // parts
    for out, own_half in ((keep, c == 0), (give, c != 0)):
        for i in range(2):
            value = jnp.where(own_half, total[i], total[2 + i])
            out[i * parts // 2 : (i + 1) * parts // 2, 0:chunk, :] = value.reshape(parts // 2, chunk, width)
        out[:, chunk:, :] = jnp.zeros((parts, out.shape[1] - chunk, width), F32)
        out[0, chunk : chunk + 1, :] = bias


def on_device(
    init_state, tiles, dst_block, rel_id, cotangent, rel_emb, w_neigh, w_self, w_gate, b_gate
):
    z, c, y, zl = lax.axis_index(Z), lax.axis_index("c"), lax.axis_index("y"), lax.axis_index("zl")
    snaps = 4
    tile, width = init_state.shape[1:]
    rows = tile // 8
    bias_row = b_gate.reshape(1, width)
    pair = (2, rows, width)
    flat = (2 * rows, width)

    own_tiles, own_cot, init = tiles[0, 0], cotangent[0, 0], init_state[0]
    here = jnp.stack([z, c, zl, y]).astype(jnp.int32)
    codes = (jnp.concatenate([here, dst_block.reshape(2), rel_id.reshape(2)]),)
    piece = (2 * rows + 8, tile)
    give, half0, half1 = local(
        give_tiles,
        codes,
        (own_tiles, init, own_cot),
        [(4, piece[0] + rows // 2, tile), (tile // 4, width), (tile // 4, width)],
        arrays_in=pltpu.HBM,
        semaphores=[pltpu.SemaphoreType.DMA((18,))],
    )
    got_tiles = swap(give)
    held, ids = [None] * snaps, [None] * snaps
    part = [local(functools.partial(cut_tiles, core), codes, (own_tiles, got_tiles), [piece] * 4) for core in range(2)]
    ring = [part[0][0]] + [along(part[0][s], Z, s) for s in range(1, 4)]
    near = [along(half0, Z, 1), along(half1, Z, -1)]
    far = [swap(v) for v in near]
    cut_cot = local(cut_rows, (here,), (own_cot, got_tiles), [pair] * 4)

    def join(core, ring):
        held[core], held[2 + core], ids[core], ids[2 + core] = local(
            join_tiles, (here,), ring, [(2, 2 * rows, tile)] * 2 + [8, 8]
        )

    join(0, ring)
    work = [(2, tile, width), (8, rows, width)]
    stored, states = [], []
    state = lines = None
    for t in range(snaps):
        if t == 0:
            *to_y, state = local(
                spread_first,
                (here, ids[0]),
                (held[0], rel_emb, init, *near, *far),
                [(2 * rows + 8, width)] * 4 + [flat],
                work,
            )
        else:
            ring = [state] + [along(state, Z, s) for s in range(1, 4)]
            (packed,) = local(pack_ring, (here,), ring, [(4, *flat)])
            to_y = local(spread_next, (here, ids[t]), [held[t], rel_emb] + ring + [swap(packed)], [flat] * 4, work)
        came_y = [to_y[0]] + [along(to_y[s], "y", s) for s in range(1, 4)]
        if t == 0:
            lines = came_y
            late = [along(part[1][s], Z, s) for s in range(1, 4)]
            join(1, [part[1][0]] + late)
        update, self_part = local(gates, (here,), (state, w_self, w_gate, bias_row), [flat] * 2)
        terms = came_y + [state, update, self_part, w_neigh]
        if t == 1:
            ring = [cut_cot[0]] + [along(cut_cot[s], Z, s) for s in range(1, 4)]
            cots = local(join_rows, (here,), ring, [pair] * 4, [(4, 2, rows, width)])
        new, agg, candidate = local(advance, (here,), terms, [flat] * 3)
        stored.append((state, agg, update, candidate))
        states.append(new)
        state = new

    cut = local(cut_states, (here,), states, [pair] * 4, [(4, 2, rows, width)])
    cut = [cut[0]] + [along(cut[s], Z, s) for s in range(1, 4)]

    d_prev = d_in = None
    pres, gates_in, rel_lines = [None] * snaps, [None] * snaps, []
    for t in reversed(range(snaps)):
        held_state, agg, update, candidate = stored[t]
        tail = (cots[t], held_state, update, candidate, w_neigh)
        outs = [flat, flat, pair, flat]
        if d_in is None:
            d_pre, d_gate, d_agg, d_keep = local(retreat_last, (here,), tail, outs)
        else:
            d_pre, d_gate, d_agg, d_keep = local(retreat, (here,), (*d_in, d_prev, *tail), outs)
        pres[t], gates_in[t] = d_pre, d_gate
        if t == 0:
            break
        pieces = [d_agg] + [along(d_agg, "y", -s) for s in range(1, 4)]
        (d_prev,) = local(before, (here,), (d_keep, d_pre, d_gate, w_self, w_gate), [flat])
        second = t == snaps - 2
        other, mine_rows, rel_rows, *mine_states = local(
            gather_back_with if second else gather_back,
            (here, ids[t]),
            [held[t]] + pieces + (cut if second else []),
            [(6 if second else 4, *pair), (4, *pair), (4, 8, width)] + [(4, rows, width)] * second,
            [(8, rows, width), flat, (tile, width)],
        )
        got = swap(other)
        if second:
            (state_out,) = local(join_states, (here,), (*mine_states, got), [(tile, width)])
        rel_lines.append(rel_rows)
        if t == 1:
            square = (width, width)
            later = local(
                functools.partial(later_grads, snaps - 1),
                (here, *ids[1:]),
                [s[0] for s in stored[1:]]
                + [s[1] for s in stored[1:]]
                + pres[1:]
                + gates_in[1:]
                + rel_lines[::-1],
                [square] * 4 + [(8, width)],
                [(4, snaps - 1, *flat)],
                flops=20_000_000_000,
            )
        parts = local(add_pairs, (here,), (mine_rows, got), [pair] * 4)
        d_in = [parts[0]] + [along(parts[s], Z, s) for s in range(1, 4)]

    parts = 16
    chunk = 2 * width // parts
    size = (parts, chunk + 8, width)
    keep, give = local(
        weight_grads, (here,), (stored[0][0], stored[0][1], d_pre, d_gate, d_agg, *lines, *later), [size] * 2
    )
    plane = ("zh", "zl", "y")
    summed = jnp.sum(lax.all_to_all(keep + swap(give), plane, 0, 0, tiled=True), axis=0)
    summed = (summed + along(summed, "b", 2)) + (along(summed, "b", 1) + along(summed, "b", 3))
    mine_sum = lax.all_to_all(jnp.broadcast_to(summed[None], size), plane, 0, 0, tiled=True)
    other_sum = swap(mine_sum)
    halves = (jnp.where(c == 0, mine_sum, other_sum), jnp.where(c == 0, other_sum, mine_sum))
    grads = [h[:, :chunk].reshape(2, width, width)[i] for h in halves for i in range(2)]
    return (state_out.reshape(1, 1, tile, width), *grads, mine_sum[0, chunk])


def solution(mesh):
    torus = Mesh(mesh.devices.reshape(2, 2, 4, 2, mesh.shape["batch"]), AXES)
    return jax.shard_map(
        on_device,
        mesh=torus,
        in_specs=(
            P("b", ENT, None),
            P("b", TM, ENT, None, None),
            P("b", TM, ENT),
            P("b", TM, ENT),
            P("b", TM, ENT, None),
            P(),
            P(),
            P(),
            P(),
            P(),
        ),
        out_specs=(P("b", TM, ENT, None), P(), P(), P(), P(), P()),
        check_vma=False,
    )
```

```python
import functools
import math

import jax
import jax.numpy as jnp
from jax import lax
from jax.experimental import pallas as pl
from jax.experimental.pallas import tpu as pltpu
from jax.sharding import Mesh
from jax.sharding import PartitionSpec as P


INTERPRET = False
VMEM_LIMIT = 16 * 1024 * 1024

AXES = ("zh", "c", "y", "zl", "b")
TM = ("zh", "c")
ENT = ("y", "zl")
Z = ("zh", "zl")
F32 = jnp.float32
BF16 = jnp.bfloat16


def halves(value):
    high = value.astype(BF16)
    return high, (value - high.astype(F32)).astype(BF16)


def product(left, right, dims=((1,), (0,))):
    (a, b), (c, d) = halves(left), halves(right)
    dot = lambda p, q: lax.dot_general(p, q, (dims, ((), ())), preferred_element_type=F32)
    return dot(a, c) + (dot(a, d) + dot(b, c))


def along(value, axis, steps):
    count = lax.axis_size(axis)
    return lax.ppermute(value, axis, [(i, (i + steps) % count) for i in range(count)])


def swap(value):
    return along(value, "c", 1)


def ring(pieces, axis, sign=1):
    far = along(pieces[2], axis, 2 * sign)
    one, three = along(pieces[1], axis, sign), along(pieces[3], axis, 3 * sign)
    return [pieces[0], one, far, three]


def local(kernel, tables, arrays, outs, scratch=(), flops=1_000_000, arrays_in=pltpu.VMEM, semaphores=()):
    vmem, smem = pl.BlockSpec(memory_space=pltpu.VMEM), pl.BlockSpec(memory_space=pltpu.SMEM)
    size = sum(a.size for a in arrays) + sum(math.prod(o) for o in outs if not isinstance(o, int))
    return pl.pallas_call(
        kernel,
        out_shape=[
            jax.ShapeDtypeStruct((o,), jnp.int32) if isinstance(o, int) else jax.ShapeDtypeStruct(o, F32)
            for o in outs
        ],
        in_specs=[smem] * len(tables) + [pl.BlockSpec(memory_space=arrays_in)] * len(arrays),
        out_specs=[smem if isinstance(o, int) else vmem for o in outs],
        scratch_shapes=[pltpu.VMEM(s, F32) for s in scratch] + list(semaphores),
        cost_estimate=pl.CostEstimate(flops=flops, bytes_accessed=4 * size, transcendentals=0),
        compiler_params=pltpu.CompilerParams(vmem_limit_bytes=VMEM_LIMIT),
        interpret=INTERPRET,
    )(*tables, *(a if arrays_in is pltpu.VMEM or INTERPRET else pltpu.with_memory_space_constraint(a, arrays_in) for a in arrays))


def ahead(z, s):
    return lax.rem(z + s, 4)


def behind(z, s):
    return lax.rem(z + 4 - s, 4)


def row(i, step):
    return pl.multiple_of(i * step, step)


def id_codes(place, lane):
    codes = jnp.zeros(lane.shape, F32)
    for j in range(2):
        codes = jnp.where(lane == 2 * j, place[4 + j].astype(F32), codes)
        codes = jnp.where(lane == 2 * j + 1, place[6 + j].astype(F32), codes)
    return codes


def give_tiles(place, own, init, cot, out, half0, half1, sems):
    c = place[1]
    rows, width = own.shape[1] // 8, init.shape[1]
    quarter = half0.shape[0]
    copies = []

    def copy(source, target):
        copies.append(pltpu.make_async_copy(source, target, sems.at[len(copies)]))
        copies[-1].start()

    for to in range(4):
        at = row(to * 2 + 1 - c, rows)
        for j in range(2):
            copy(own.at[j, pl.ds(at, rows), :], out.at[to, j * rows : (j + 1) * rows, :])
        for i in range(2):
            copy(
                cot.at[pl.ds(row(4 * to + 2 - 2 * c + i, rows // 2), rows // 2), :],
                out.at[to, 2 * rows + 8 :, i * width : (i + 1) * width],
            )
    copy(init.at[pl.ds(row(2 * c, quarter), quarter), :], half0)
    copy(init.at[pl.ds(row(2 * c + 1, quarter), quarter), :], half1)
    lane = lax.broadcasted_iota(jnp.int32, (8, own.shape[2]), 1) // 128
    codes = id_codes(place, lane)
    for to in range(4):
        out[to, 2 * rows : 2 * rows + 8, :] = codes
    for waited in copies:
        waited.wait()


def cut_tiles(core, place, own, got, *outs):
    z, c = place[0], place[1]
    rows = own.shape[1] // 8
    lane = lax.broadcasted_iota(jnp.int32, (8, own.shape[2]), 1) // 128

    @pl.when(c == core)
    def _():
        codes = id_codes(place, lane)
        for s in range(4):
            to = ahead(z, s)
            for j in range(2):
                outs[s][j * rows : (j + 1) * rows, :] = own[j, pl.ds(row(to * 2 + c, rows), rows), :]
            outs[s][2 * rows :, :] = codes

    @pl.when(c != core)
    def _():
        for s in range(4):
            outs[s][...] = got[ahead(z, s), 0 : 2 * rows + 8, :]


def join_tiles(place, p0, p1, p2, p3, early, late, early_ids, late_ids):
    z, y = place[0], place[3]
    rows = early.shape[1]
    pieces = (p0, p1, p2, p3)
    codes = [
        [jnp.max(piece[rows : rows + 8, q * 128 : (q + 1) * 128]).astype(jnp.int32) for q in range(4)] for piece in pieces
    ]
    for s, piece in enumerate(pieces):
        from_z = behind(z, s)
        b = lax.rem(from_z, 2)

        def write(tiles, ids):
            tiles[b] = piece[0:rows, :]
            for j in range(2):
                dst, rel = codes[s][2 * j], codes[s][2 * j + 1]
                ids[2 * b + j] = lax.rem(lax.div(dst, 2) + 4 - y, 4) * 2 + lax.rem(dst, 2)
                ids[4 + 2 * b + j] = rel

        pl.when(from_z < 2)(functools.partial(write, early, early_ids))
        pl.when(from_z >= 2)(functools.partial(write, late, late_ids))


def spread(ids, tiles, rel_emb, full, slots):
    rows = tiles.shape[1] // 2
    slots[...] = jnp.zeros_like(slots)

    def step(b, carry):
        block = tiles[b]
        part = product(block, full[b])
        sums = jnp.sum(block, axis=1, keepdims=True)
        for j in range(2):
            line = rel_emb[pl.ds(ids[4 + 2 * b + j], 1), :]
            slots[ids[2 * b + j]] += part[j * rows : (j + 1) * rows] + sums[j * rows : (j + 1) * rows] * line
        return carry

    lax.fori_loop(0, 2, step, 0)


def spread_first(place, ids, tiles, rel_emb, init, near0, near1, far0, far1, o0, o1, o2, o3, own, full, slots):
    z, c, zl = place[0], place[1], place[2]
    quarter = near0.shape[0]
    rows = tiles.shape[1] // 2
    full[zl] = init[...]
    for i, (near, far) in enumerate(((near0, far0), (near1, far1))):
        full[1 - zl, pl.ds(row(2 * c + i, quarter), quarter), :] = near[...]
        full[1 - zl, pl.ds(row(2 - 2 * c + i, quarter), quarter), :] = far[...]
    at = row(z * 2 + c, rows)
    for b in range(2):
        own[b * rows : (b + 1) * rows, :] = full[b, pl.ds(at, rows), :]
    spread(ids, tiles, rel_emb, full, slots)
    ones = jnp.ones((8, tiles.shape[2]), F32)
    lane = lax.broadcasted_iota(jnp.int32, (1, o0.shape[1]), 1)
    for s, out in enumerate((o0, o1, o2, o3)):
        out[0 : 2 * rows, :] = slots[2 * s : 2 * s + 2].reshape(2 * rows, -1)
        out[2 * rows :, :] = jnp.full((8, out.shape[1]), -1.0, F32)
    for b in range(2):
        sums = product(ones, tiles[b], ((1,), (1,)))
        for j in range(2):
            k = 2 * b + j
            line = jnp.where(lane == rows, ids[k].astype(F32), ids[4 + k].astype(F32))
            for out in (o0, o1, o2, o3):
                out[2 * rows + k : 2 * rows + k + 1, :] = line
                out[2 * rows + k : 2 * rows + k + 1, 0:rows] = sums[0:1, j * rows : (j + 1) * rows]


def pack_ring(place, p0, p1, p2, p3, out):
    rows = out.shape[1]
    for s, piece in enumerate((p0, p1, p2, p3)):
        out[s] = piece[0:rows, :]


def spread_next(place, ids, tiles, rel_emb, p0, p1, p2, p3, other, o0, o1, o2, o3, full, slots):
    z, c = place[0], place[1]
    rows = tiles.shape[1] // 2
    for s, piece in enumerate((p0, p1, p2, p3)):
        from_z = behind(z, s)
        for b in range(2):
            part = slice(b * rows, (b + 1) * rows)
            full[b, pl.ds(row(from_z * 2 + c, rows), rows), :] = piece[part, :]
            full[b, pl.ds(row(from_z * 2 + 1 - c, rows), rows), :] = other[s, part, :]
    spread(ids, tiles, rel_emb, full, slots)
    for s, out in enumerate((o0, o1, o2, o3)):
        out[...] = slots[2 * s : 2 * s + 2].reshape(2 * rows, -1)


def gates(place, state, w_self, w_gate, b_gate, update, self_part):
    held = state[...]
    update[...] = jax.nn.sigmoid(product(held, w_gate[...]) + b_gate[...])
    self_part[...] = product(held, w_self[...])


def advance(place, a0, a1, a2, a3, state, update, self_part, w_neigh, new, agg, candidate):
    rows = state.shape[0]
    total = (a0[0:rows, :] + a1[0:rows, :]) + (a2[0:rows, :] + a3[0:rows, :])
    agg[...] = total
    cand = jnp.tanh(product(total, w_neigh[...]) + self_part[...])
    candidate[...] = cand
    gate = update[...]
    new[...] = gate * cand + (1.0 - gate) * state[...]


def retreat_math(d_new, state, update, candidate, w_neigh, d_pre, d_gate, d_agg, d_keep):
    gate, cand = update[...], candidate[...]
    rest = 1.0 - gate
    pre = d_new * gate * (1.0 - cand * cand)
    d_pre[...] = pre
    d_gate[...] = d_new * (cand - state[...]) * gate * rest
    d_agg[...] = product(pre, w_neigh[...], ((1,), (1,))).reshape(d_agg.shape)
    if d_keep is not None:
        d_keep[...] = d_new * rest


def retreat_last(place, cot, state, update, candidate, w_neigh, d_pre, d_gate, d_agg, d_keep):
    d_new = cot[...].reshape(state.shape)
    retreat_math(d_new, state, update, candidate, w_neigh, d_pre, d_gate, d_agg, d_keep)


def retreat(place, d0, d1, d2, d3, d_prev, cot, state, update, candidate, w_neigh, d_pre, d_gate, d_agg, d_keep):
    came = ((d0[0:2] + d1[0:2]) + (d2[0:2] + d3[0:2]) + cot[...]).reshape(state.shape)
    retreat_math(came + d_prev[...], state, update, candidate, w_neigh, d_pre, d_gate, d_agg, d_keep)


def before(place, d_keep, d_pre, d_gate, w_self, w_gate, d_prev):
    d_prev[...] = (
        d_keep[...]
        + product(d_pre[...], w_self[...], ((1,), (1,)))
        + product(d_gate[...], w_gate[...], ((1,), (1,)))
    )


def gather_back(place, ids, tiles, g0, g1, g2, g3, other, mine, rel_rows, held, res, full):
    z, c = place[0], place[1]
    rows = g0.shape[1]
    for s, piece in enumerate((g0, g1, g2, g3)):
        held[2 * s : 2 * s + 2] = piece[...]

    def step(b, carry):
        block = tiles[b]
        sums = jnp.sum(block, axis=1, keepdims=True)
        for j in range(2):
            value = held[ids[2 * b + j]]
            res[j * rows : (j + 1) * rows, :] = value
            total = jnp.sum(sums[j * rows : (j + 1) * rows] * value, axis=0, keepdims=True)
            rel_rows[2 * b + j] = jnp.broadcast_to(total, rel_rows.shape[1:])
        full[...] = product(block, res[...], ((0,), (0,)))
        for s in range(4):
            to = ahead(z, s)
            mine[s, b] = full[pl.ds(row(to * 2 + c, rows), rows), :]
            other[s, b] = full[pl.ds(row(to * 2 + 1 - c, rows), rows), :]
        return carry

    lax.fori_loop(0, 2, step, 0)


def gather_back_with(place, ids, tiles, g0, g1, g2, g3, s0, s1, s2, s3, other, mine, rel_rows, states, held, res, full):
    c = place[1]
    gather_back(place, ids, tiles, g0, g1, g2, g3, other, mine, rel_rows, held, res, full)
    for s, piece in enumerate((s0, s1, s2, s3)):
        states[s] = piece[c]
        other[4 + s // 2, s % 2] = piece[1 - c]


def add_pairs(place, mine, got, n0, n1, n2, n3):
    for s, out in enumerate((n0, n1, n2, n3)):
        out[...] = mine[s] + got[s]


def cut_rows(place, own, got, *outs):
    z, c = place[0], place[1]
    rows, width = own.shape[0] // 8, own.shape[1]
    for s in range(4):
        to = ahead(z, s)
        outs[s][c] = own[pl.ds(row(to * 2 + c, rows), rows), :]
        outs[s][1 - c, 0 : rows // 2] = got[to, 2 * rows + 8 :, 0:width]
        outs[s][1 - c, rows // 2 :] = got[to, 2 * rows + 8 :, width:]


def join_rows(place, p0, p1, p2, p3, *refs):
    outs, stack = refs[:4], refs[4]
    z = place[0]
    for s, piece in enumerate((p0, p1, p2, p3)):
        stack[behind(z, s)] = piece[...]
    for t in range(4):
        for b in range(2):
            outs[t][b] = stack[(t // 2) * 2 + b, t % 2]


def cut_states(place, n0, n1, n2, n3, *refs):
    outs, stack = refs[:4], refs[4]
    z = place[0]
    rows = outs[0].shape[1]
    for t, state in enumerate((n0, n1, n2, n3)):
        for b in range(2):
            stack[(t // 2) * 2 + b, t % 2] = state[b * rows : (b + 1) * rows, :]
    for s in range(4):
        outs[s][...] = stack[ahead(z, s)]


def join_states(place, mine, got, out):
    z, c = place[0], place[1]
    rows = mine.shape[1]
    for s in range(4):
        from_z = behind(z, s)
        out[pl.ds(row(from_z * 2 + c, rows), rows), :] = mine[s]
        out[pl.ds(row(from_z * 2 + 1 - c, rows), rows), :] = got[4 + s // 2, s % 2]


def dense_grads(state, agg, pre, gate_in):
    pairs = ((agg, pre), (state, pre), (state, gate_in))
    return [product(a, b, ((0,), (0,))) for a, b in pairs], jnp.sum(gate_in, axis=0, keepdims=True)


def later_grads(count, place, *refs):
    tables, refs = refs[:count], refs[count:]
    lines, outs, stack = refs[4 * count : 5 * count], refs[5 * count : 5 * count + 5], refs[-1]
    for kind in range(4):
        for i in range(count):
            stack[kind, i] = refs[kind * count + i][...]
    for out in outs:
        out[...] = jnp.zeros_like(out)

    def step(i, carry):
        total, bias = dense_grads(stack[0, i], stack[1, i], stack[2, i], stack[3, i])
        for out, value in zip(outs[1:4], total):
            out[...] += value
        outs[4][...] += jnp.broadcast_to(bias, outs[4].shape)
        return carry

    lax.fori_loop(0, count, step, 0)
    for ids, line in zip(tables, lines):
        for k in range(4):
            outs[0][pl.ds(ids[4 + k], 1), :] += line[k, 0:1, :]


def weight_grads(place, state, agg, pre, gate_in, d_agg, l0, l1, l2, l3, *refs):
    later, d_bias, keep, give = refs[:4], refs[4], refs[5], refs[6]
    c = place[1]
    rows, width = d_agg.shape[1:]
    total, bias = dense_grads(state[...], agg[...], pre[...], gate_in[...])
    d_rel = later[0][...]
    relation = lax.broadcasted_iota(jnp.int32, (8, width), 1).astype(F32)
    for s, piece in enumerate((l0, l1, l2, l3)):
        line = piece[2 * rows :, 0:128]
        slot, rel, sums = line[:, rows : rows + 1], line[:, rows + 1 : rows + 2], line[:, 0:rows]
        found = sum(
            product(jnp.where(slot == float(2 * s + b), sums, 0.0), d_agg[b]) for b in range(2)
        )
        d_rel = d_rel + product((rel == relation).astype(F32), found, ((0,), (0,)))
    total = [d_rel] + [a + b[...] for a, b in zip(total, later[1:])]
    bias = bias + d_bias[0:1, :]
    parts = keep.shape[0]
    chunk = 2 * width // parts
    for out, own_half in ((keep, c == 0), (give, c != 0)):
        for i in range(2):
            value = jnp.where(own_half, total[i], total[2 + i])
            out[i * parts // 2 : (i + 1) * parts // 2, 0:chunk, :] = value.reshape(parts // 2, chunk, width)
        out[:, chunk:, :] = jnp.zeros((parts, out.shape[1] - chunk, width), F32)
        out[0, chunk : chunk + 1, :] = bias


def on_device(
    init_state, tiles, dst_block, rel_id, cotangent, rel_emb, w_neigh, w_self, w_gate, b_gate
):
    z, c, y, zl = lax.axis_index(Z), lax.axis_index("c"), lax.axis_index("y"), lax.axis_index("zl")
    snaps = 4
    tile, width = init_state.shape[1:]
    rows = tile // 8
    bias_row = b_gate.reshape(1, width)
    pair = (2, rows, width)
    flat = (2 * rows, width)

    own_tiles, own_cot, init = tiles[0, 0], cotangent[0, 0], init_state[0]
    here = jnp.stack([z, c, zl, y]).astype(jnp.int32)
    codes = (jnp.concatenate([here, dst_block.reshape(2), rel_id.reshape(2)]),)
    piece = (2 * rows + 8, tile)
    give, half0, half1 = local(
        give_tiles,
        codes,
        (own_tiles, init, own_cot),
        [(4, piece[0] + rows // 2, tile), (tile // 4, width), (tile // 4, width)],
        arrays_in=pltpu.HBM,
        semaphores=[pltpu.SemaphoreType.DMA((18,))],
    )
    got_tiles = swap(give)
    held, ids = [None] * snaps, [None] * snaps
    part = [local(functools.partial(cut_tiles, core), codes, (own_tiles, got_tiles), [piece] * 4) for core in range(2)]
    tiles_ring = ring(part[0], Z)
    near = [along(half0, Z, 1), along(half1, Z, -1)]
    far = [swap(v) for v in near]
    cut_cot = local(cut_rows, (here,), (own_cot, got_tiles), [pair] * 4)

    def join(core, came):
        held[core], held[2 + core], ids[core], ids[2 + core] = local(
            join_tiles, (here,), came, [(2, 2 * rows, tile)] * 2 + [8, 8]
        )

    join(0, tiles_ring)
    work = [(2, tile, width), (8, rows, width)]
    stored, states = [], []
    state = lines = None
    for t in range(snaps):
        if t == 0:
            *to_y, state = local(
                spread_first,
                (here, ids[0]),
                (held[0], rel_emb, init, *near, *far),
                [(2 * rows + 8, width)] * 4 + [flat],
                work,
            )
        else:
            came_z = ring([state] * 4, Z)
            (packed,) = local(pack_ring, (here,), came_z, [(4, *flat)])
            to_y = local(spread_next, (here, ids[t]), [held[t], rel_emb] + came_z + [swap(packed)], [flat] * 4, work)
        came_y = ring(to_y, "y")
        if t == 0:
            lines = came_y
            join(1, ring(part[1], Z))
        update, self_part = local(gates, (here,), (state, w_self, w_gate, bias_row), [flat] * 2)
        terms = came_y + [state, update, self_part, w_neigh]
        if t == 1:
            cots = local(join_rows, (here,), ring(cut_cot, Z), [pair] * 4, [(4, 2, rows, width)])
        new, agg, candidate = local(advance, (here,), terms, [flat] * 3)
        stored.append((state, agg, update, candidate))
        states.append(new)
        state = new

    cut = local(cut_states, (here,), states, [pair] * 4, [(4, 2, rows, width)])
    cut = ring(cut, Z)

    d_prev = d_in = None
    pres, gates_in, rel_lines = [None] * snaps, [None] * snaps, []
    for t in reversed(range(snaps)):
        held_state, agg, update, candidate = stored[t]
        tail = (cots[t], held_state, update, candidate, w_neigh)
        outs = [flat, flat, pair, flat]
        if d_in is None:
            d_pre, d_gate, d_agg, d_keep = local(retreat_last, (here,), tail, outs)
        else:
            d_pre, d_gate, d_agg, d_keep = local(retreat, (here,), (*d_in, d_prev, *tail), outs)
        pres[t], gates_in[t] = d_pre, d_gate
        if t == 0:
            break
        pieces = ring([d_agg] * 4, "y", -1)
        (d_prev,) = local(before, (here,), (d_keep, d_pre, d_gate, w_self, w_gate), [flat])
        second = t == snaps - 2
        other, mine_rows, rel_rows, *mine_states = local(
            gather_back_with if second else gather_back,
            (here, ids[t]),
            [held[t]] + pieces + (cut if second else []),
            [(6 if second else 4, *pair), (4, *pair), (4, 8, width)] + [(4, rows, width)] * second,
            [(8, rows, width), flat, (tile, width)],
        )
        got = swap(other)
        if second:
            (state_out,) = local(join_states, (here,), (*mine_states, got), [(tile, width)])
        rel_lines.append(rel_rows)
        if t == 1:
            square = (width, width)
            later = local(
                functools.partial(later_grads, snaps - 1),
                (here, *ids[1:]),
                [s[0] for s in stored[1:]]
                + [s[1] for s in stored[1:]]
                + pres[1:]
                + gates_in[1:]
                + rel_lines[::-1],
                [square] * 4 + [(8, width)],
                [(4, snaps - 1, *flat)],
                flops=20_000_000_000,
            )
        parts = local(add_pairs, (here,), (mine_rows, got), [pair] * 4)
        d_in = ring(parts, Z)

    parts = 16
    chunk = 2 * width // parts
    size = (parts, chunk + 8, width)
    keep, give = local(
        weight_grads, (here,), (stored[0][0], stored[0][1], d_pre, d_gate, d_agg, *lines, *later), [size] * 2
    )
    plane = ("zh", "zl", "y")
    summed = jnp.sum(lax.all_to_all(keep + swap(give), plane, 0, 0, tiled=True), axis=0)
    came_x = ring([summed] * 4, "b")
    summed = (came_x[0] + came_x[2]) + (came_x[1] + came_x[3])
    mine_sum = lax.all_to_all(jnp.broadcast_to(summed[None], size), plane, 0, 0, tiled=True)
    other_sum = swap(mine_sum)
    halves = (jnp.where(c == 0, mine_sum, other_sum), jnp.where(c == 0, other_sum, mine_sum))
    grads = [h[:, :chunk].reshape(2, width, width)[i] for h in halves for i in range(2)]
    return (state_out.reshape(1, 1, tile, width), *grads, mine_sum[0, chunk])


def solution(mesh):
    torus = Mesh(mesh.devices.reshape(2, 2, 4, 2, mesh.shape["batch"]), AXES)
    return jax.shard_map(
        on_device,
        mesh=torus,
        in_specs=(
            P("b", ENT, None),
            P("b", TM, ENT, None, None),
            P("b", TM, ENT),
            P("b", TM, ENT),
            P("b", TM, ENT, None),
            P(),
            P(),
            P(),
            P(),
            P(),
        ),
        out_specs=(P("b", TM, ENT, None), P(), P(), P(), P(), P()),
        check_vma=False,
    )
```

```python
import functools
import math

import jax
import jax.numpy as jnp
from jax import lax
from jax.experimental import pallas as pl
from jax.experimental.pallas import tpu as pltpu
from jax.sharding import Mesh
from jax.sharding import PartitionSpec as P


INTERPRET = False
VMEM_LIMIT = 16 * 1024 * 1024

AXES = ("zh", "c", "y", "zl", "b")
TM = ("zh", "c")
ENT = ("y", "zl")
Z = ("zh", "zl")
F32 = jnp.float32
BF16 = jnp.bfloat16


def halves(value):
    high = value.astype(BF16)
    return high, (value - high.astype(F32)).astype(BF16)


def product(left, right, dims=((1,), (0,))):
    (a, b), (c, d) = halves(left), halves(right)
    dot = lambda p, q: lax.dot_general(p, q, (dims, ((), ())), preferred_element_type=F32)
    return dot(a, c) + (dot(a, d) + dot(b, c))


def along(value, axis, steps):
    count = lax.axis_size(axis)
    return lax.ppermute(value, axis, [(i, (i + steps) % count) for i in range(count)])


def swap(value):
    return along(value, "c", 1)


def ring(pieces, axis, sign=1):
    far = along(pieces[2], axis, 2 * sign)
    one, three = along(pieces[1], axis, sign), along(pieces[3], axis, 3 * sign)
    return [pieces[0], one, far, three]


def local(kernel, tables, arrays, outs, scratch=(), flops=1_000_000, arrays_in=pltpu.VMEM, semaphores=()):
    vmem, smem = pl.BlockSpec(memory_space=pltpu.VMEM), pl.BlockSpec(memory_space=pltpu.SMEM)
    size = sum(a.size for a in arrays) + sum(math.prod(o) for o in outs if not isinstance(o, int))
    return pl.pallas_call(
        kernel,
        out_shape=[
            jax.ShapeDtypeStruct((o,), jnp.int32) if isinstance(o, int) else jax.ShapeDtypeStruct(o, F32)
            for o in outs
        ],
        in_specs=[smem] * len(tables) + [pl.BlockSpec(memory_space=arrays_in)] * len(arrays),
        out_specs=[smem if isinstance(o, int) else vmem for o in outs],
        scratch_shapes=[pltpu.VMEM(s, F32) for s in scratch] + list(semaphores),
        cost_estimate=pl.CostEstimate(flops=flops, bytes_accessed=4 * size, transcendentals=0),
        compiler_params=pltpu.CompilerParams(vmem_limit_bytes=VMEM_LIMIT),
        interpret=INTERPRET,
    )(*tables, *(a if arrays_in is pltpu.VMEM or INTERPRET else pltpu.with_memory_space_constraint(a, arrays_in) for a in arrays))


def ahead(z, s):
    return lax.rem(z + s, 4)


def behind(z, s):
    return lax.rem(z + 4 - s, 4)


def row(i, step):
    return pl.multiple_of(i * step, step)


def id_codes(place, lane):
    codes = jnp.zeros(lane.shape, F32)
    for j in range(2):
        codes = jnp.where(lane == 2 * j, place[4 + j].astype(F32), codes)
        codes = jnp.where(lane == 2 * j + 1, place[6 + j].astype(F32), codes)
    return codes


def give_tiles(place, own, init, cot, out, half0, half1, sems):
    c = place[1]
    rows, width = own.shape[1] // 8, init.shape[1]
    quarter = half0.shape[0]
    copies = []

    def copy(source, target):
        copies.append(pltpu.make_async_copy(source, target, sems.at[len(copies)]))
        copies[-1].start()

    for to in range(4):
        at = row(to * 2 + 1 - c, rows)
        for j in range(2):
            copy(own.at[j, pl.ds(at, rows), :], out.at[to, j * rows : (j + 1) * rows, :])
        for i in range(2):
            copy(
                cot.at[pl.ds(row(4 * to + 2 - 2 * c + i, rows // 2), rows // 2), :],
                out.at[to, 2 * rows + 8 :, i * width : (i + 1) * width],
            )
    copy(init.at[pl.ds(row(2 * c, quarter), quarter), :], half0)
    copy(init.at[pl.ds(row(2 * c + 1, quarter), quarter), :], half1)
    lane = lax.broadcasted_iota(jnp.int32, (8, own.shape[2]), 1) // 128
    codes = id_codes(place, lane)
    for to in range(4):
        out[to, 2 * rows : 2 * rows + 8, :] = codes
    for waited in copies:
        waited.wait()


def cut_tiles(core, place, own, got, *outs):
    z, c = place[0], place[1]
    rows = own.shape[1] // 8
    lane = lax.broadcasted_iota(jnp.int32, (8, own.shape[2]), 1) // 128

    @pl.when(c == core)
    def _():
        codes = id_codes(place, lane)
        for s in range(4):
            to = ahead(z, s)
            for j in range(2):
                outs[s][j * rows : (j + 1) * rows, :] = own[j, pl.ds(row(to * 2 + c, rows), rows), :]
            outs[s][2 * rows :, :] = codes

    @pl.when(c != core)
    def _():
        for s in range(4):
            outs[s][...] = got[ahead(z, s), 0 : 2 * rows + 8, :]


def join_tiles(place, p0, p1, p2, p3, early, late, early_ids, late_ids):
    z, y = place[0], place[3]
    rows = early.shape[1]
    pieces = (p0, p1, p2, p3)
    codes = [
        [jnp.max(piece[rows : rows + 8, q * 128 : (q + 1) * 128]).astype(jnp.int32) for q in range(4)] for piece in pieces
    ]
    for s, piece in enumerate(pieces):
        from_z = behind(z, s)
        b = lax.rem(from_z, 2)

        def write(tiles, ids):
            tiles[b] = piece[0:rows, :]
            for j in range(2):
                dst, rel = codes[s][2 * j], codes[s][2 * j + 1]
                ids[2 * b + j] = lax.rem(lax.div(dst, 2) + 4 - y, 4) * 2 + lax.rem(dst, 2)
                ids[4 + 2 * b + j] = rel

        pl.when(from_z < 2)(functools.partial(write, early, early_ids))
        pl.when(from_z >= 2)(functools.partial(write, late, late_ids))


def spread(ids, tiles, rel_emb, full, slots):
    rows = tiles.shape[1] // 2
    slots[...] = jnp.zeros_like(slots)

    def step(b, carry):
        block = tiles[b]
        part = product(block, full[b])
        sums = jnp.sum(block, axis=1, keepdims=True)
        for j in range(2):
            line = rel_emb[pl.ds(ids[4 + 2 * b + j], 1), :]
            slots[ids[2 * b + j]] += part[j * rows : (j + 1) * rows] + sums[j * rows : (j + 1) * rows] * line
        return carry

    lax.fori_loop(0, 2, step, 0)


def spread_first(place, ids, tiles, rel_emb, init, near0, near1, far0, far1, o0, o1, o2, o3, own, full, slots):
    z, c, zl = place[0], place[1], place[2]
    quarter = near0.shape[0]
    rows = tiles.shape[1] // 2
    full[zl] = init[...]
    for i, (near, far) in enumerate(((near0, far0), (near1, far1))):
        full[1 - zl, pl.ds(row(2 * c + i, quarter), quarter), :] = near[...]
        full[1 - zl, pl.ds(row(2 - 2 * c + i, quarter), quarter), :] = far[...]
    at = row(z * 2 + c, rows)
    for b in range(2):
        own[b * rows : (b + 1) * rows, :] = full[b, pl.ds(at, rows), :]
    spread(ids, tiles, rel_emb, full, slots)
    ones = jnp.ones((8, tiles.shape[2]), F32)
    lane = lax.broadcasted_iota(jnp.int32, (1, o0.shape[1]), 1)
    for s, out in enumerate((o0, o1, o2, o3)):
        out[0 : 2 * rows, :] = slots[2 * s : 2 * s + 2].reshape(2 * rows, -1)
        out[2 * rows :, :] = jnp.full((8, out.shape[1]), -1.0, F32)
    for b in range(2):
        sums = product(ones, tiles[b], ((1,), (1,)))
        for j in range(2):
            k = 2 * b + j
            line = jnp.where(lane == rows, ids[k].astype(F32), ids[4 + k].astype(F32))
            for out in (o0, o1, o2, o3):
                out[2 * rows + k : 2 * rows + k + 1, :] = line
                out[2 * rows + k : 2 * rows + k + 1, 0:rows] = sums[0:1, j * rows : (j + 1) * rows]


def pack_ring(place, p0, p1, p2, p3, out):
    rows = out.shape[1]
    for s, piece in enumerate((p0, p1, p2, p3)):
        out[s] = piece[0:rows, :]


def spread_next(place, ids, tiles, rel_emb, p0, p1, p2, p3, other, o0, o1, o2, o3, full, slots):
    z, c = place[0], place[1]
    rows = tiles.shape[1] // 2
    for s, piece in enumerate((p0, p1, p2, p3)):
        from_z = behind(z, s)
        for b in range(2):
            part = slice(b * rows, (b + 1) * rows)
            full[b, pl.ds(row(from_z * 2 + c, rows), rows), :] = piece[part, :]
            full[b, pl.ds(row(from_z * 2 + 1 - c, rows), rows), :] = other[s, part, :]
    spread(ids, tiles, rel_emb, full, slots)
    for s, out in enumerate((o0, o1, o2, o3)):
        out[...] = slots[2 * s : 2 * s + 2].reshape(2 * rows, -1)


def gates(place, state, w_self, w_gate, b_gate, update, self_part):
    held = state[...]
    update[...] = jax.nn.sigmoid(product(held, w_gate[...]) + b_gate[...])
    self_part[...] = product(held, w_self[...])


def advance(place, a0, a1, a2, a3, state, update, self_part, w_neigh, new, agg, candidate):
    rows = state.shape[0]
    total = (a0[0:rows, :] + a1[0:rows, :]) + (a2[0:rows, :] + a3[0:rows, :])
    agg[...] = total
    cand = jnp.tanh(product(total, w_neigh[...]) + self_part[...])
    candidate[...] = cand
    gate = update[...]
    new[...] = gate * cand + (1.0 - gate) * state[...]


def retreat_math(d_new, state, update, candidate, w_neigh, d_pre, d_gate, d_agg, d_keep):
    gate, cand = update[...], candidate[...]
    rest = 1.0 - gate
    pre = d_new * gate * (1.0 - cand * cand)
    d_pre[...] = pre
    d_gate[...] = d_new * (cand - state[...]) * gate * rest
    d_agg[...] = product(pre, w_neigh[...], ((1,), (1,))).reshape(d_agg.shape)
    if d_keep is not None:
        d_keep[...] = d_new * rest


def retreat_last(cot, state, update, candidate, w_neigh, d_pre, d_gate, d_agg, d_keep):
    d_new = cot[...].reshape(state.shape)
    retreat_math(d_new, state, update, candidate, w_neigh, d_pre, d_gate, d_agg, d_keep)


def retreat(place, d0, d1, d2, d3, d_prev, cot, state, update, candidate, w_neigh, d_pre, d_gate, d_agg, d_keep):
    came = ((d0[0:2] + d1[0:2]) + (d2[0:2] + d3[0:2]) + cot[...]).reshape(state.shape)
    retreat_math(came + d_prev[...], state, update, candidate, w_neigh, d_pre, d_gate, d_agg, d_keep)


def turn(place, a0, a1, a2, a3, state, update, self_part, w_neigh, cot, new, agg, cand, d_pre, d_gate, d_agg, d_keep):
    advance(place, a0, a1, a2, a3, state, update, self_part, w_neigh, new, agg, cand)
    retreat_last(cot, state, update, cand, w_neigh, d_pre, d_gate, d_agg, d_keep)


def before(place, d_keep, d_pre, d_gate, w_self, w_gate, d_prev):
    d_prev[...] = (
        d_keep[...]
        + product(d_pre[...], w_self[...], ((1,), (1,)))
        + product(d_gate[...], w_gate[...], ((1,), (1,)))
    )


def gather_back(place, ids, tiles, g0, g1, g2, g3, other, mine, rel_rows, held, res, full):
    z, c = place[0], place[1]
    rows = g0.shape[1]
    for s, piece in enumerate((g0, g1, g2, g3)):
        held[2 * s : 2 * s + 2] = piece[...]

    def step(b, carry):
        block = tiles[b]
        sums = jnp.sum(block, axis=1, keepdims=True)
        for j in range(2):
            value = held[ids[2 * b + j]]
            res[j * rows : (j + 1) * rows, :] = value
            total = jnp.sum(sums[j * rows : (j + 1) * rows] * value, axis=0, keepdims=True)
            rel_rows[2 * b + j] = jnp.broadcast_to(total, rel_rows.shape[1:])
        full[...] = product(block, res[...], ((0,), (0,)))
        for s in range(4):
            to = ahead(z, s)
            mine[s, b] = full[pl.ds(row(to * 2 + c, rows), rows), :]
            other[s, b] = full[pl.ds(row(to * 2 + 1 - c, rows), rows), :]
        return carry

    lax.fori_loop(0, 2, step, 0)


def gather_back_with(place, ids, tiles, g0, g1, g2, g3, s0, s1, s2, s3, other, mine, rel_rows, states, held, res, full):
    c = place[1]
    gather_back(place, ids, tiles, g0, g1, g2, g3, other, mine, rel_rows, held, res, full)
    for s, piece in enumerate((s0, s1, s2, s3)):
        states[s] = piece[c]
        other[4 + s // 2, s % 2] = piece[1 - c]


def add_pairs(place, mine, got, n0, n1, n2, n3):
    for s, out in enumerate((n0, n1, n2, n3)):
        out[...] = mine[s] + got[s]


def cut_rows(place, own, got, *outs):
    z, c = place[0], place[1]
    rows, width = own.shape[0] // 8, own.shape[1]
    for s in range(4):
        to = ahead(z, s)
        outs[s][c] = own[pl.ds(row(to * 2 + c, rows), rows), :]
        outs[s][1 - c, 0 : rows // 2] = got[to, 2 * rows + 8 :, 0:width]
        outs[s][1 - c, rows // 2 :] = got[to, 2 * rows + 8 :, width:]


def join_rows(place, p0, p1, p2, p3, *refs):
    outs, stack = refs[:4], refs[4]
    z = place[0]
    for s, piece in enumerate((p0, p1, p2, p3)):
        stack[behind(z, s)] = piece[...]
    for t in range(4):
        for b in range(2):
            outs[t][b] = stack[(t // 2) * 2 + b, t % 2]


def cut_states(place, n0, n1, n2, n3, *refs):
    outs, stack = refs[:4], refs[4]
    z = place[0]
    rows = outs[0].shape[1]
    for t, state in enumerate((n0, n1, n2, n3)):
        for b in range(2):
            stack[(t // 2) * 2 + b, t % 2] = state[b * rows : (b + 1) * rows, :]
    for s in range(4):
        outs[s][...] = stack[ahead(z, s)]


def join_states(place, mine, got, out):
    z, c = place[0], place[1]
    rows = mine.shape[1]
    for s in range(4):
        from_z = behind(z, s)
        out[pl.ds(row(from_z * 2 + c, rows), rows), :] = mine[s]
        out[pl.ds(row(from_z * 2 + 1 - c, rows), rows), :] = got[4 + s // 2, s % 2]


def dense_grads(state, agg, pre, gate_in):
    pairs = ((agg, pre), (state, pre), (state, gate_in))
    return [product(a, b, ((0,), (0,))) for a, b in pairs], jnp.sum(gate_in, axis=0, keepdims=True)


def later_grads(count, place, *refs):
    tables, refs = refs[:count], refs[count:]
    lines, outs, stack = refs[4 * count : 5 * count], refs[5 * count : 5 * count + 5], refs[-1]
    for kind in range(4):
        for i in range(count):
            stack[kind, i] = refs[kind * count + i][...]
    for out in outs:
        out[...] = jnp.zeros_like(out)

    def step(i, carry):
        total, bias = dense_grads(stack[0, i], stack[1, i], stack[2, i], stack[3, i])
        for out, value in zip(outs[1:4], total):
            out[...] += value
        outs[4][...] += jnp.broadcast_to(bias, outs[4].shape)
        return carry

    lax.fori_loop(0, count, step, 0)
    for ids, line in zip(tables, lines):
        for k in range(4):
            outs[0][pl.ds(ids[4 + k], 1), :] += line[k, 0:1, :]


def weight_grads(place, state, agg, pre, gate_in, d_agg, l0, l1, l2, l3, *refs):
    later, d_bias, keep, give = refs[:4], refs[4], refs[5], refs[6]
    c = place[1]
    rows, width = d_agg.shape[1:]
    total, bias = dense_grads(state[...], agg[...], pre[...], gate_in[...])
    d_rel = later[0][...]
    relation = lax.broadcasted_iota(jnp.int32, (8, width), 1).astype(F32)
    for s, piece in enumerate((l0, l1, l2, l3)):
        line = piece[2 * rows :, 0:128]
        slot, rel, sums = line[:, rows : rows + 1], line[:, rows + 1 : rows + 2], line[:, 0:rows]
        found = sum(
            product(jnp.where(slot == float(2 * s + b), sums, 0.0), d_agg[b]) for b in range(2)
        )
        d_rel = d_rel + product((rel == relation).astype(F32), found, ((0,), (0,)))
    total = [d_rel] + [a + b[...] for a, b in zip(total, later[1:])]
    bias = bias + d_bias[0:1, :]
    parts = keep.shape[0]
    chunk = 2 * width // parts
    for out, own_half in ((keep, c == 0), (give, c != 0)):
        for i in range(2):
            value = jnp.where(own_half, total[i], total[2 + i])
            out[i * parts // 2 : (i + 1) * parts // 2, 0:chunk, :] = value.reshape(parts // 2, chunk, width)
        out[:, chunk:, :] = jnp.zeros((parts, out.shape[1] - chunk, width), F32)
        out[0, chunk : chunk + 1, :] = bias


def finish(place, *refs):
    ins, (agg, *lines_later), (keep, give), kept = refs[:10], refs[10:20], refs[20:22], refs[22:]
    retreat(place, *ins, *kept)
    weight_grads(place, ins[6], agg, *kept[:3], *lines_later, keep, give)


def on_device(
    init_state, tiles, dst_block, rel_id, cotangent, rel_emb, w_neigh, w_self, w_gate, b_gate
):
    z, c, y, zl = lax.axis_index(Z), lax.axis_index("c"), lax.axis_index("y"), lax.axis_index("zl")
    snaps = 4
    tile, width = init_state.shape[1:]
    rows = tile // 8
    bias_row = b_gate.reshape(1, width)
    pair = (2, rows, width)
    flat = (2 * rows, width)

    own_tiles, own_cot, init = tiles[0, 0], cotangent[0, 0], init_state[0]
    here = jnp.stack([z, c, zl, y]).astype(jnp.int32)
    codes = (jnp.concatenate([here, dst_block.reshape(2), rel_id.reshape(2)]),)
    piece = (2 * rows + 8, tile)
    give, half0, half1 = local(
        give_tiles,
        codes,
        (own_tiles, init, own_cot),
        [(4, piece[0] + rows // 2, tile), (tile // 4, width), (tile // 4, width)],
        arrays_in=pltpu.HBM,
        semaphores=[pltpu.SemaphoreType.DMA((18,))],
    )
    got_tiles = swap(give)
    held, ids = [None] * snaps, [None] * snaps
    part = [local(functools.partial(cut_tiles, core), codes, (own_tiles, got_tiles), [piece] * 4) for core in range(2)]
    tiles_ring = ring(part[0], Z)
    near = [along(half0, Z, 1), along(half1, Z, -1)]
    far = [swap(v) for v in near]
    cut_cot = local(cut_rows, (here,), (own_cot, got_tiles), [pair] * 4)

    def join(core, came):
        held[core], held[2 + core], ids[core], ids[2 + core] = local(
            join_tiles, (here,), came, [(2, 2 * rows, tile)] * 2 + [8, 8]
        )

    join(0, tiles_ring)
    work = [(2, tile, width), (8, rows, width)]
    stored, states = [], []
    state = lines = None
    for t in range(snaps):
        if t == 0:
            *to_y, state = local(
                spread_first,
                (here, ids[0]),
                (held[0], rel_emb, init, *near, *far),
                [(2 * rows + 8, width)] * 4 + [flat],
                work,
            )
        else:
            came_z = ring([state] * 4, Z)
            (packed,) = local(pack_ring, (here,), came_z, [(4, *flat)])
            to_y = local(spread_next, (here, ids[t]), [held[t], rel_emb] + came_z + [swap(packed)], [flat] * 4, work)
        came_y = ring(to_y, "y")
        if t == 0:
            lines = came_y
            join(1, ring(part[1], Z))
        update, self_part = local(gates, (here,), (state, w_self, w_gate, bias_row), [flat] * 2)
        terms = came_y + [state, update, self_part, w_neigh]
        if t == 1:
            cots = local(join_rows, (here,), ring(cut_cot, Z), [pair] * 4, [(4, 2, rows, width)])
        if t + 1 < snaps:
            new, agg, candidate = local(advance, (here,), terms, [flat] * 3)
        else:
            new, agg, candidate, *turned = local(turn, (here,), terms + [cots[t]], [flat] * 5 + [pair, flat])
        stored.append((state, agg, update, candidate))
        states.append(new)
        state = new

    cut = local(cut_states, (here,), states, [pair] * 4, [(4, 2, rows, width)])
    cut = ring(cut, Z)

    d_prev = d_in = None
    pres, gates_in, rel_lines = [None] * snaps, [None] * snaps, []
    for t in reversed(range(snaps)):
        held_state, agg, update, candidate = stored[t]
        tail = (cots[t], held_state, update, candidate, w_neigh)
        outs = [flat, flat, pair, flat]
        if t == 0:
            break
        if d_in is None:
            d_pre, d_gate, d_agg, d_keep = turned
        else:
            d_pre, d_gate, d_agg, d_keep = local(retreat, (here,), (*d_in, d_prev, *tail), outs)
        pres[t], gates_in[t] = d_pre, d_gate
        pieces = ring([d_agg] * 4, "y", -1)
        (d_prev,) = local(before, (here,), (d_keep, d_pre, d_gate, w_self, w_gate), [flat])
        second = t == snaps - 2
        other, mine_rows, rel_rows, *mine_states = local(
            gather_back_with if second else gather_back,
            (here, ids[t]),
            [held[t]] + pieces + (cut if second else []),
            [(6 if second else 4, *pair), (4, *pair), (4, 8, width)] + [(4, rows, width)] * second,
            [(8, rows, width), flat, (tile, width)],
        )
        got = swap(other)
        if second:
            (state_out,) = local(join_states, (here,), (*mine_states, got), [(tile, width)])
        rel_lines.append(rel_rows)
        if t == 1:
            square = (width, width)
            later = local(
                functools.partial(later_grads, snaps - 1),
                (here, *ids[1:]),
                [s[0] for s in stored[1:]]
                + [s[1] for s in stored[1:]]
                + pres[1:]
                + gates_in[1:]
                + rel_lines[::-1],
                [square] * 4 + [(8, width)],
                [(4, snaps - 1, *flat)],
                flops=20_000_000_000,
            )
        parts = local(add_pairs, (here,), (mine_rows, got), [pair] * 4)
        d_in = ring(parts, Z)

    parts = 16
    chunk = 2 * width // parts
    size = (parts, chunk + 8, width)
    keep, give = local(
        finish, (here,), (*d_in, d_prev, *tail, stored[0][1], *lines, *later), [size] * 2, [flat, flat, pair, flat]
    )
    plane = ("zh", "zl", "y")
    summed = jnp.sum(lax.all_to_all(keep + swap(give), plane, 0, 0, tiled=True), axis=0)
    came_x = ring([summed] * 4, "b")
    summed = (came_x[0] + came_x[2]) + (came_x[1] + came_x[3])
    mine_sum = lax.all_to_all(jnp.broadcast_to(summed[None], size), plane, 0, 0, tiled=True)
    other_sum = swap(mine_sum)
    halves = (jnp.where(c == 0, mine_sum, other_sum), jnp.where(c == 0, other_sum, mine_sum))
    grads = [h[:, :chunk].reshape(2, width, width)[i] for h in halves for i in range(2)]
    return (state_out.reshape(1, 1, tile, width), *grads, mine_sum[0, chunk])


def solution(mesh):
    torus = Mesh(mesh.devices.reshape(2, 2, 4, 2, mesh.shape["batch"]), AXES)
    return jax.shard_map(
        on_device,
        mesh=torus,
        in_specs=(
            P("b", ENT, None),
            P("b", TM, ENT, None, None),
            P("b", TM, ENT),
            P("b", TM, ENT),
            P("b", TM, ENT, None),
            P(),
            P(),
            P(),
            P(),
            P(),
        ),
        out_specs=(P("b", TM, ENT, None), P(), P(), P(), P(), P()),
        check_vma=False,
    )
```
